128 devices in a mesh: dp: 1, ep: 128 (over z, y, x, core).
Axes of the slice: x: 4, y: 4, z: 4, core: 2. Of those that a mesh axis runs over, the one named last changes fastest.
Arguments:
- x_in: bfloat16 [32768, 2048], P(('dp', 'ep'))
- norm_gain: bfloat16 [2048], replicated
- w_router: bfloat16 [2048, 128], replicated
- expert_ids: int32 [32768, 8], P(('dp', 'ep'))
- w_gate: bfloat16 [128, 2048, 768], P('ep')
- w_up: bfloat16 [128, 2048, 768], P('ep')
- w_down: bfloat16 [128, 768, 2048], P('ep')
Outputs:
- output: bfloat16 [32768, 2048], P(('dp', 'ep'))
All inputs are finite; a program needn't handle non-finite values.
Results may differ from the reference program's by a relative error of at most 0.00693909.
Values are sent between devices in bfloat16 or wider.
A program may use at most 1 GiB of HBM per device.

```python
import jax
import jax.numpy as jnp
from jax import lax

HIDDEN = 2048
EXPERT_FF = 768
EXPERTS = 128
TOP_K = 8
TOKENS = 256
GROUP_SIZE = 128

EPS = 1e-6
CAP_DEV = 2 * TOKENS * TOP_K // EXPERTS
HOT_COUNT = EXPERTS // 4
COLD_LEFT = TOKENS * TOP_K - HOT_COUNT * CAP_DEV
COLD_BASE = COLD_LEFT // (EXPERTS - HOT_COUNT)
COLD_EXTRA = COLD_LEFT % (EXPERTS - HOT_COUNT)
ROW_LIMIT = GROUP_SIZE * CAP_DEV


def draw_device(hot_flag, key):
    key_rank, key_rows, key_cols = jax.random.split(key, 3)
    expert_range = jnp.arange(EXPERTS, dtype=jnp.int32)
    noise = jax.random.randint(key_rank, (EXPERTS,), 0, EXPERTS, dtype=jnp.int32)
    score = (1 - hot_flag) * (EXPERTS * EXPERTS) + noise * EXPERTS + expert_range
    rank = jnp.argsort(jnp.argsort(score))
    counts = jnp.where(rank < HOT_COUNT, CAP_DEV, COLD_BASE + (rank - HOT_COUNT < COLD_EXTRA).astype(jnp.int32))
    bounds = jnp.cumsum(counts).astype(jnp.int32)
    flat_ids = jnp.searchsorted(bounds, jnp.arange(TOKENS * TOP_K, dtype=jnp.int32), side="right").astype(jnp.int32)
    table = flat_ids.reshape(TOP_K, TOKENS).T
    table = jax.random.permutation(key_rows, table, axis=0)
    col_score = jax.random.randint(key_cols, (TOKENS, TOP_K), 0, TOP_K, dtype=jnp.int32) * TOP_K + jnp.arange(TOP_K, dtype=jnp.int32)
    col_order = jnp.argsort(col_score, axis=1)
    return jnp.take_along_axis(table, col_order, axis=1)


def draw_routes(key):
    key_hot, key_dev = jax.random.split(key)
    hot_order = jax.random.permutation(key_hot, EXPERTS)
    hot_flag = (jnp.argsort(hot_order) < HOT_COUNT).astype(jnp.int32)
    dev_keys = jax.random.split(key_dev, GROUP_SIZE)
    routes = jax.vmap(draw_device, in_axes=(None, 0))(hot_flag, dev_keys)
    return routes.reshape(GROUP_SIZE * TOKENS, TOP_K).astype(jnp.int32)


def setup_inputs(seed: int = 0, part: int = 0) -> dict:
    shared = jax.random.split(jax.random.key(seed), 5)
    own = jax.random.split(jax.random.fold_in(jax.random.key(seed + 1), part), 2)
    x_in = (0.5 * jax.random.normal(own[0], (GROUP_SIZE * TOKENS, HIDDEN), jnp.float32)).astype(jnp.bfloat16)
    norm_gain = jax.random.uniform(shared[0], (HIDDEN,), jnp.float32, 0.5, 1.5).astype(jnp.bfloat16)
    w_router = (2.0 * HIDDEN ** -0.5 * jax.random.normal(shared[1], (HIDDEN, EXPERTS), jnp.float32)).astype(jnp.bfloat16)
    w_gate = (HIDDEN ** -0.5 * jax.random.normal(shared[2], (EXPERTS, HIDDEN, EXPERT_FF), jnp.float32)).astype(jnp.bfloat16)
    w_up = (HIDDEN ** -0.5 * jax.random.normal(shared[3], (EXPERTS, HIDDEN, EXPERT_FF), jnp.float32)).astype(jnp.bfloat16)
    w_down = (1.5 * EXPERT_FF ** -0.5 * jax.random.normal(shared[4], (EXPERTS, EXPERT_FF, HIDDEN), jnp.float32)).astype(jnp.bfloat16)
    expert_ids = draw_routes(own[1])
    return {"x_in": x_in, "norm_gain": norm_gain, "w_router": w_router, "expert_ids": expert_ids, "w_gate": w_gate, "w_up": w_up, "w_down": w_down}


def reference(x_in, norm_gain, w_router, expert_ids, w_gate, w_up, w_down):
    resid = x_in.astype(jnp.float32)
    mean_sq = jnp.mean(resid * resid, axis=-1, keepdims=True)
    normed = (resid * lax.rsqrt(mean_sq + EPS) * norm_gain.astype(jnp.float32)).astype(jnp.bfloat16)
    logits = jnp.dot(normed, w_router, preferred_element_type=jnp.float32)
    router_p = jax.nn.softmax(logits, axis=-1)
    picked = jnp.take_along_axis(router_p, expert_ids, axis=1)
    gates = picked / jnp.sum(picked, axis=1, keepdims=True)
    total = x_in.shape[0]

    def one_expert(moe_sum, inputs):
        expert, gate_w, up_w, down_w = inputs
        hits = expert_ids == expert
        weight = jnp.sum(jnp.where(hits, gates, 0.0), axis=1)
        rows = jnp.nonzero(jnp.any(hits, axis=1), size=ROW_LIMIT, fill_value=total)[0]
        sel_rows = jnp.take(normed, rows, axis=0, mode="fill", fill_value=0)
        gate_val = jnp.dot(sel_rows, gate_w, preferred_element_type=jnp.float32)
        up_val = jnp.dot(sel_rows, up_w, preferred_element_type=jnp.float32)
        hidden_act = (jax.nn.silu(gate_val) * up_val).astype(jnp.bfloat16)
        out_rows = jnp.dot(hidden_act, down_w, preferred_element_type=jnp.float32).astype(jnp.bfloat16)
        row_w = jnp.take(weight, rows, mode="fill", fill_value=0)
        moe_sum = moe_sum.at[rows].add(out_rows.astype(jnp.float32) * row_w[:, None], mode="drop")
        return moe_sum, None

    start_sum = jnp.zeros((total, HIDDEN), jnp.float32)
    moe_sum = lax.scan(one_expert, start_sum, (jnp.arange(EXPERTS, dtype=jnp.int32), w_gate, w_up, w_down))[0]
    return (resid + moe_sum).astype(jnp.bfloat16)
```

```python
import functools

import jax
import jax.numpy as jnp
from jax import lax
from jax.experimental import pallas as pl
from jax.experimental.pallas import tpu as pltpu
from jax.sharding import PartitionSpec as P

EPS = 1e-6
SLOTS = 32
F32, BF16 = jnp.float32, jnp.bfloat16


def route_kernel(x_ref, gain_ref, wr_ref, ids_ref, idst_ref, h_ref, gate_ref, pos_ref, post_ref):
    tokens, experts = gate_ref.shape[1], gate_ref.shape[2]
    top_k = ids_ref.shape[1]
    resid = x_ref[...].astype(F32)
    mean_sq = jnp.mean(resid * resid, axis=-1, keepdims=True)
    normed = (resid * lax.rsqrt(mean_sq + EPS) * gain_ref[...].astype(F32)).astype(BF16)
    h_ref[...] = normed
    logits = jnp.dot(normed, wr_ref[...], preferred_element_type=F32)
    exps = jnp.exp(logits - jnp.max(logits, axis=-1, keepdims=True))
    router_p = exps / jnp.sum(exps, axis=-1, keepdims=True)

    lane_expert = lax.broadcasted_iota(jnp.int32, (tokens, experts), 1)
    chosen = jnp.zeros((tokens, experts), F32)
    row_expert = lax.broadcasted_iota(jnp.int32, (experts, tokens), 0)
    chosen_t = jnp.zeros((experts, tokens), F32)
    for j in range(top_k):
        chosen += jnp.where(ids_ref[:, j:j + 1] == lane_expert, 1.0, 0.0)
        chosen_t += jnp.where(idst_ref[j:j + 1, :] == row_expert, 1.0, 0.0)

    picked = router_p * chosen
    gates = picked / jnp.sum(picked, axis=-1, keepdims=True)
    part0 = gates.astype(BF16)
    rest = gates - part0.astype(F32)
    part1 = rest.astype(BF16)
    part2 = (rest - part1.astype(F32)).astype(BF16)
    gate_ref[0] = part0
    gate_ref[1] = part1
    gate_ref[2] = part2

    rows = lax.broadcasted_iota(jnp.int32, (tokens, tokens), 0)
    cols = lax.broadcasted_iota(jnp.int32, (tokens, tokens), 1)
    lower = jnp.where(cols < rows, 1.0, 0.0).astype(BF16)
    upper = jnp.where(rows < cols, 1.0, 0.0).astype(BF16)
    pos = jnp.dot(lower, chosen.astype(BF16), preferred_element_type=F32)
    pos_t = jnp.dot(chosen_t.astype(BF16), upper, preferred_element_type=F32)
    pos_ref[...] = jnp.where(chosen > 0.0, pos, 255.0).astype(BF16)
    post_ref[...] = jnp.where(chosen_t > 0.0, pos_t, 255.0)


def pack_kernel(slots, h_ref, post_ref, out_ref):
    group, tokens = post_ref.shape
    slot = lax.broadcasted_iota(jnp.int32, (group, slots, tokens), 1).astype(F32)
    pick = jnp.where(post_ref[...][:, None, :] == slot, 1.0, 0.0).astype(BF16)
    rows = jnp.dot(pick.reshape(group * slots, tokens), h_ref[...], preferred_element_type=F32).astype(BF16)
    out_ref[...] = rows


def mlp_kernel(x_ref, wg_ref, wu_ref, wd_ref, y_ref):
    rows = x_ref[...]
    gate_val = jnp.dot(rows, wg_ref[0], preferred_element_type=F32)
    up_val = jnp.dot(rows, wu_ref[0], preferred_element_type=F32)
    act = (jax.nn.silu(gate_val) * up_val).astype(BF16)
    y_ref[...] = jnp.dot(act, wd_ref[0], preferred_element_type=F32).astype(BF16)


def combine_kernel(slots, gate_ref, pos_ref, y_ref, base_ref, out_ref, acc_ref):
    step = pl.program_id(0)
    width = y_ref.shape[0]
    tokens, experts = pos_ref.shape

    @pl.when(step == 0)
    def _():
        acc_ref[...] = base_ref[...].astype(F32)

    expert = lax.broadcasted_iota(jnp.int32, (experts, width), 0)
    column = lax.broadcasted_iota(jnp.int32, (experts, width), 1) + step * width
    spread = jnp.where(column // slots == expert, 1.0, 0.0).astype(BF16)
    gates = gate_ref[...].reshape(3 * tokens, experts)
    wide_gate = jnp.dot(gates, spread, preferred_element_type=F32).reshape(3, tokens, width)
    wide_pos = jnp.dot(pos_ref[...], spread, preferred_element_type=F32)
    slot = (lax.broadcasted_iota(jnp.int32, (tokens, width), 1) % slots).astype(F32)
    hit = (wide_pos == slot)[None]
    weight = jnp.where(hit, wide_gate, 0.0).astype(BF16).reshape(3 * tokens, width)
    sums = jnp.dot(weight, y_ref[...], preferred_element_type=F32)
    acc_ref[...] += sums[:tokens] + sums[tokens:2 * tokens] + sums[2 * tokens:]

    @pl.when(step == pl.num_programs(0) - 1)
    def _():
        out_ref[...] = acc_ref[...].astype(out_ref.dtype)


def params(**kw):
    return pltpu.CompilerParams(vmem_limit_bytes=60 * 2 ** 20, **kw)


def cost(flops, nbytes):
    return pl.CostEstimate(flops=int(flops), bytes_accessed=int(nbytes), transcendentals=0)


def route(x_in, norm_gain, w_router, expert_ids):
    tokens, hidden = x_in.shape
    experts = w_router.shape[1]
    shape = jax.ShapeDtypeStruct
    return pl.pallas_call(
        route_kernel,
        out_shape=(shape((tokens, hidden), BF16), shape((3, tokens, experts), BF16), shape((tokens, experts), BF16), shape((experts, tokens), F32)),
        compiler_params=params(),
        cost_estimate=cost(2 * tokens * hidden * experts, 4 * tokens * hidden),
        name="route",
    )(x_in, norm_gain.reshape(1, hidden), w_router, expert_ids, expert_ids.T)


def pack(h, pos_t, slots, group):
    tokens, hidden = h.shape
    experts = pos_t.shape[0]
    return pl.pallas_call(
        functools.partial(pack_kernel, slots),
        grid=(experts // group,),
        out_shape=jax.ShapeDtypeStruct((experts * slots, hidden), BF16),
        in_specs=[pl.BlockSpec((tokens, hidden), lambda i: (0, 0)), pl.BlockSpec((group, tokens), lambda i: (i, 0))],
        out_specs=pl.BlockSpec((group * slots, hidden), lambda i: (i, 0)),
        compiler_params=params(),
        cost_estimate=cost(2 * experts * slots * tokens * hidden, 2 * experts * slots * hidden),
        name="pack",
    )(h, pos_t)


def exchange(rows, devices):
    blocks = rows.reshape(devices, rows.shape[0] // devices, rows.shape[1])
    return lax.all_to_all(blocks, "ep", 0, 0, tiled=True).reshape(rows.shape)


def mlp(rows, w_gate, w_up, w_down, block):
    total, hidden = rows.shape
    ff = w_gate.shape[2]
    whole = lambda i: (0, 0, 0)
    row_spec = pl.BlockSpec((block, hidden), lambda i: (i, 0))
    return pl.pallas_call(
        mlp_kernel,
        grid=(total // block,),
        out_shape=jax.ShapeDtypeStruct(rows.shape, BF16),
        in_specs=[row_spec, pl.BlockSpec((1, hidden, ff), whole), pl.BlockSpec((1, hidden, ff), whole), pl.BlockSpec((1, ff, hidden), whole)],
        out_specs=row_spec,
        compiler_params=params(),
        cost_estimate=cost(6 * total * hidden * ff, 4 * total * hidden + 6 * hidden * ff),
        name="mlp",
    )(rows, w_gate, w_up, w_down)


def combine(gates, pos, rows, resid, slots, block):
    total, hidden = rows.shape
    tokens, experts = pos.shape
    return pl.pallas_call(
        functools.partial(combine_kernel, slots),
        grid=(total // block,),
        out_shape=jax.ShapeDtypeStruct((tokens, hidden), BF16),
        in_specs=[
            pl.BlockSpec((3, tokens, experts), lambda i: (0, 0, 0)),
            pl.BlockSpec((tokens, experts), lambda i: (0, 0)),
            pl.BlockSpec((block, hidden), lambda i: (i, 0)),
            pl.BlockSpec((tokens, hidden), lambda i: (0, 0)),
        ],
        out_specs=pl.BlockSpec((tokens, hidden), lambda i: (0, 0)),
        scratch_shapes=[pltpu.VMEM((tokens, hidden), F32)],
        compiler_params=params(),
        cost_estimate=cost(6 * tokens * total * hidden, 2 * total * hidden),
        name="combine",
    )(gates, pos, rows, resid)


def solution(mesh):
    def local_block(x_in, norm_gain, w_router, expert_ids, w_gate, w_up, w_down):
        tokens, hidden = x_in.shape
        experts = w_router.shape[1]
        h, gates, pos, pos_t = route(x_in, norm_gain, w_router, expert_ids)
        outgoing = pack(h, pos_t, SLOTS, 16)
        received = exchange(outgoing, experts)
        y = mlp(received, w_gate, w_up, w_down, 512)
        returned = exchange(y, experts)
        return combine(gates, pos, returned, x_in, SLOTS, 512)

    tok_spec = P(("dp", "ep"), None)
    expert_spec = P("ep", None, None)
    return jax.shard_map(local_block, mesh=mesh, in_specs=(tok_spec, P(None), P(None, None), tok_spec, expert_spec, expert_spec, expert_spec), out_specs=tok_spec, check_vma=False)
```

```python
import functools

import jax
import jax.numpy as jnp
from jax import lax
from jax.experimental import pallas as pl
from jax.experimental.pallas import tpu as pltpu
from jax.sharding import PartitionSpec as P

EPS = 1e-6
SLOTS = 32
SIDE = 4
STRIDES = (2, 8, 32)
WIDTHS = (768, 640, 640)
STARTS = (0, 768, 1408)
PLANE = 32
F32, BF16, I32 = jnp.float32, jnp.bfloat16, jnp.int32
MESH = pl.DeviceIdType.MESH


def shifted(dev, axis, step):
    stride = STRIDES[axis]
    here = lax.rem(lax.div(dev, stride), SIDE)
    return dev + (lax.rem(here + step, SIDE) - here) * stride


def plane_axes(axis):
    return tuple(a for a in (2, 1, 0) if a != axis)


def in_plane(dev, axis, p):
    a, b = plane_axes(axis)
    dev = shifted(shifted(dev, a, lax.div(p, 8)), b, lax.rem(lax.div(p, 2), SIDE))
    core = lax.rem(dev, 2)
    return dev + lax.rem(core + lax.rem(p, 2), 2) - core


def opposite(p):
    da, db = lax.div(p, 8), lax.rem(lax.div(p, 2), SIDE)
    return lax.rem(SIDE - da, SIDE) * 8 + lax.rem(SIDE - db, SIDE) * 2 + lax.rem(p, 2)


def relative(axis, along, p):
    a, b = plane_axes(axis)
    place = {axis: along, a: lax.div(p, 8), b: lax.rem(lax.div(p, 2), SIDE)}
    return (place[2] * SIDE + place[1]) * 8 + place[0] * 2 + lax.rem(p, 2)


def split_relative(axis, rho):
    place = (lax.rem(lax.div(rho, 2), SIDE), lax.rem(lax.div(rho, 8), SIDE), lax.div(rho, 32))
    a, b = plane_axes(axis)
    return place[axis], place[a] * 8 + place[b] * 2 + lax.rem(rho, 2)


def remote(src, dst, send_sem, recv_sem, dev):
    return pltpu.make_async_remote_copy(src, dst, send_sem, recv_sem, device_id={"ep": dev}, device_id_type=MESH)


def wait_for(ref, sem):
    pltpu.make_async_copy(ref, ref, sem).wait()


def source(axis, r):
    return 0 if r == 0 else 3 * axis + r


def route_kernel(x_ref, gain_ref, wr_ref, ids_ref, idst_ref, h_ref, gate_ref):
    tokens, experts = x_ref.shape[0], wr_ref.shape[1]
    top_k = ids_ref.shape[1]
    resid = x_ref[...].astype(F32)
    mean_sq = jnp.mean(resid * resid, axis=-1, keepdims=True)
    normed = (resid * lax.rsqrt(mean_sq + EPS) * gain_ref[...].astype(F32)).astype(BF16)
    h_ref[...] = normed
    logits = jnp.dot(normed, wr_ref[...], preferred_element_type=F32)
    exps = jnp.exp(logits - jnp.max(logits, axis=-1, keepdims=True))
    router_p = exps / jnp.sum(exps, axis=-1, keepdims=True)
    lane_expert = lax.broadcasted_iota(I32, (tokens, experts), 1)
    chosen = jnp.zeros((tokens, experts), F32)
    for j in range(top_k):
        chosen += jnp.where(ids_ref[:, j:j + 1] == lane_expert, 1.0, 0.0)
    picked = router_p * chosen
    gates_t = jnp.transpose(picked / jnp.sum(picked, axis=-1, keepdims=True))
    row_expert = lax.broadcasted_iota(I32, (experts, tokens), 0)
    for j in range(top_k):
        gate_ref[j:j + 1, :] = jnp.sum(jnp.where(idst_ref[j:j + 1, :] == row_expert, gates_t, 0.0), axis=0, keepdims=True)


def dispatch_kernel(h_ref, ids_ref, gate_ref, post_ref, gates_ref, recv0, recv1, recv2,
                    line0, line1, line2, ids_scr, gate_scr, pack0, pack1, pack2,
                    line_send, line_recv, ids_send, ids_recv, gate_send, gate_recv, send_sem, recv_sem, local_sem):
    recv, line, pack = (recv0, recv1, recv2), (line0, line1, line2), (pack0, pack1, pack2)
    top_k, tokens = ids_ref.shape
    experts = post_ref.shape[1]
    me = lax.axis_index("ep")
    for r in (1, 3, 2):
        for axis in range(3):
            dev, k = shifted(me, axis, r), source(axis, SIDE - r)
            n = k - 1
            remote(ids_ref, ids_scr.at[n], ids_send, ids_recv.at[n], dev).start()
            remote(gate_ref, gate_scr.at[n], gate_send, gate_recv.at[n], dev).start()
            cols = h_ref.at[:, pl.ds(STARTS[axis], WIDTHS[axis])]
            remote(cols, line[axis].at[SIDE - r - 1], line_send.at[axis], line_recv.at[n], dev).start()

    row_expert = lax.broadcasted_iota(I32, (experts, tokens), 0)
    rows = lax.broadcasted_iota(I32, (tokens, tokens), 0)
    upper = jnp.where(rows < lax.broadcasted_iota(I32, (tokens, tokens), 1), 1.0, 0.0).astype(BF16)
    slot = lax.broadcasted_iota(I32, (SLOTS, tokens), 0).astype(F32)

    def tables(k, ids, gates):
        chosen = jnp.zeros((experts, tokens), F32)
        dense = jnp.zeros((experts, tokens), F32)
        for j in range(top_k):
            hit = ids[j:j + 1, :] == row_expert
            chosen += jnp.where(hit, 1.0, 0.0)
            dense += jnp.where(hit, gates[j:j + 1, :], 0.0)
        before = jnp.dot(chosen.astype(BF16), upper, preferred_element_type=F32)
        post_ref[k] = jnp.where(chosen > 0.0, before, 255.0)
        gates_ref[k] = dense

    for r in (0, 1, 3, 2):
        for axis in range(3):
            k = source(axis, r)
            if r == 0 and axis == 0:
                tables(0, ids_ref[...], gate_ref[...])
            elif r > 0:
                wait_for(ids_scr.at[k - 1], ids_recv.at[k - 1])
                wait_for(gate_scr.at[k - 1], gate_recv.at[k - 1])
                tables(k, ids_scr[k - 1], gate_scr[k - 1])
                wait_for(line[axis].at[r - 1], line_recv.at[k - 1])

        def chunk(q, carry, r=r):
            for axis in range(3):
                k = source(axis, r)
                picks = []
                for j in range(8):
                    expert = in_plane(me, axis, q * 8 + j)
                    picks.append(jnp.where(post_ref[k, pl.ds(expert, 1), :] == slot, 1.0, 0.0).astype(BF16))
                if r == 0:
                    own = h_ref[:, STARTS[axis]:STARTS[axis] + WIDTHS[axis]]
                else:
                    own = line[axis][r - 1]
                packed = jnp.dot(jnp.concatenate(picks, axis=0), own, preferred_element_type=F32).astype(BF16)
                pack[axis][pl.ds((r * 4 + q) * 8, 8)] = packed.reshape(8, SLOTS, WIDTHS[axis])

            def send(j, c):
                p = q * 8 + j
                for axis in range(3):
                    src = pack[axis].at[r * PLANE + p]
                    dst = recv[axis].at[relative(axis, r, opposite(p))]

                    @pl.when(p == 0)
                    def _():
                        pltpu.make_async_copy(src, dst, local_sem.at[axis, r]).start()

                    @pl.when(p != 0)
                    def _():
                        remote(src, dst, send_sem.at[axis], recv_sem.at[axis], in_plane(me, axis, p)).start()
                return c

            lax.fori_loop(0, 8, send, 0)
            return carry

        lax.fori_loop(0, 4, chunk, 0)

    wait_for(ids_scr, ids_send)
    wait_for(gate_scr, gate_send)
    far = SIDE * (PLANE - 1)
    for axis in range(3):
        wait_for(line[axis], line_send.at[axis])
        for r in range(SIDE):
            wait_for(recv[axis].at[0], local_sem.at[axis, r])
        wait_for(pack[axis].at[pl.ds(0, far)], send_sem.at[axis])
        wait_for(recv[axis].at[pl.ds(0, far)], recv_sem.at[axis])


def expert_kernel(block, x0, x1, x2, wg_ref, wu_ref, wd_ref, ret0, ret1, ret2,
                  in0, in1, in2, out0, out1, out2, load_sem, send_sem, recv_sem, local_sem):
    x, ret, held, done = (x0, x1, x2), (ret0, ret1, ret2), (in0, in1, in2), (out0, out1, out2)
    me = lax.axis_index("ep")
    blocks = x0.shape[0] // block

    def load(b, axis):
        part = pl.ds(b * block, block)
        return pltpu.make_async_copy(x[axis].at[part], held[axis].at[part], load_sem.at[axis, b])

    for b in range(blocks):
        for axis in range(3):
            load(b, axis).start()

    def step(b, carry):
        for axis in range(3):
            load(b, axis).wait()
        gate_val, up_val = 0.0, 0.0
        for axis in range(3):
            rows = held[axis][pl.ds(b * block, block)].reshape(block * SLOTS, WIDTHS[axis])
            span = slice(STARTS[axis], STARTS[axis] + WIDTHS[axis])
            gate_val += jnp.dot(rows, wg_ref[0, span, :], preferred_element_type=F32)
            up_val += jnp.dot(rows, wu_ref[0, span, :], preferred_element_type=F32)
        act = (jax.nn.silu(gate_val) * up_val).astype(BF16)
        for axis in range(3):
            span = slice(STARTS[axis], STARTS[axis] + WIDTHS[axis])
            y = jnp.dot(act, wd_ref[0, :, span], preferred_element_type=F32).astype(BF16)
            done[axis][pl.ds(b * block, block)] = y.reshape(block, SLOTS, WIDTHS[axis])

        def send(j, c):
            rho = b * block + j
            for axis in range(3):
                along, p = split_relative(axis, rho)
                src = done[axis].at[rho]
                dst = ret[axis].at[along * PLANE + opposite(p)]

                @pl.when(p == 0)
                def _():
                    pltpu.make_async_copy(src, dst, local_sem.at[axis, along]).start()

                @pl.when(p != 0)
                def _():
                    remote(src, dst, send_sem.at[axis], recv_sem.at[axis], in_plane(me, axis, p)).start()
            return c

        lax.fori_loop(0, block, send, 0)
        return carry

    lax.fori_loop(0, blocks, step, 0)
    far = SIDE * (PLANE - 1)
    for axis in range(3):
        for r in range(SIDE):
            wait_for(ret[axis].at[0], local_sem.at[axis, r])
        wait_for(done[axis].at[pl.ds(0, far)], send_sem.at[axis])
        wait_for(ret[axis].at[pl.ds(0, far)], recv_sem.at[axis])


def combine_kernel(x_ref, post_ref, gates_ref, y0, y1, y2, out_ref,
                   in0, in1, in2, sum0, sum1, sum2, part0, part1, part2, load_sem, send_sem, recv_sem):
    y, held, sums, parts = (y0, y1, y2), (in0, in1, in2), (sum0, sum1, sum2), (part0, part1, part2)
    tokens = x_ref.shape[0]
    experts = post_ref.shape[1]
    me = lax.axis_index("ep")
    half = PLANE // 2
    width = half * SLOTS
    order = (1, 3, 2, 0)

    def load(axis, r):
        part = pl.ds(r * PLANE, PLANE)
        return pltpu.make_async_copy(y[axis].at[part], held[axis].at[part], load_sem.at[axis, r])

    for r in order:
        for axis in range(3):
            load(axis, r).start()

    expert = lax.broadcasted_iota(I32, (experts, width), 0)
    column = lax.broadcasted_iota(I32, (experts, width), 1)
    slot = (lax.broadcasted_iota(I32, (tokens, width), 1) % SLOTS).astype(F32)

    def copy(axis, r):
        return remote(sums[axis].at[r], parts[axis].at[SIDE - r - 1], send_sem.at[axis, r - 1], recv_sem.at[axis, SIDE - r - 1], shifted(me, axis, r))

    for r in order:
        for axis in range(3):
            k = source(axis, r)
            gates = jnp.transpose(gates_ref[k])
            high = gates.astype(BF16)
            rest = gates - high.astype(F32)
            mid = rest.astype(BF16)
            low = (rest - mid.astype(F32)).astype(BF16)
            table = jnp.concatenate([high, mid, low, jnp.transpose(post_ref[k]).astype(BF16)], axis=0)
            load(axis, r).wait()

            def chunk(c, carry, r=r, axis=axis, table=table):
                spread = jnp.where(in_plane(me, axis, column // SLOTS + c * half) == expert, 1.0, 0.0).astype(BF16)
                wide = jnp.dot(table, spread, preferred_element_type=F32)
                hit = wide[3 * tokens:] == slot
                weight = jnp.concatenate([jnp.where(hit, wide[i * tokens:(i + 1) * tokens], 0.0).astype(BF16) for i in range(3)], axis=0)
                rows = held[axis][pl.ds(r * PLANE + c * half, half)].reshape(width, WIDTHS[axis])
                got = jnp.dot(weight, rows, preferred_element_type=F32)
                total = got[:tokens] + got[tokens:2 * tokens] + got[2 * tokens:]

                @pl.when(c == 0)
                def _():
                    sums[axis][r] = total

                @pl.when(c != 0)
                def _():
                    sums[axis][r] += total
                return carry

            lax.fori_loop(0, 2, chunk, 0)
        if r > 0:
            for axis in range(3):
                copy(axis, r).start()

    for axis in range(3):
        span = slice(STARTS[axis], STARTS[axis] + WIDTHS[axis])
        total = x_ref[:, span].astype(F32) + sums[axis][0]
        for r in range(1, SIDE):
            wait_for(parts[axis].at[r - 1], recv_sem.at[axis, r - 1])
            total += parts[axis][r - 1]
        out_ref[:, span] = total.astype(out_ref.dtype)
    for axis in range(3):
        for r in range(1, SIDE):
            wait_for(sums[axis].at[r], send_sem.at[axis, r - 1])


def params(**kw):
    return pltpu.CompilerParams(vmem_limit_bytes=62 * 2 ** 20, **kw)


VMEM = pl.BlockSpec(memory_space=pltpu.VMEM)
ANY = pl.BlockSpec(memory_space=pl.ANY)
DMA = pltpu.SemaphoreType.DMA
shape = jax.ShapeDtypeStruct


def route(x_in, norm_gain, w_router, expert_ids):
    tokens, hidden = x_in.shape
    top_k = expert_ids.shape[1]
    return pl.pallas_call(
        route_kernel,
        out_shape=(shape((tokens, hidden), BF16), shape((top_k, tokens), F32)),
        compiler_params=params(),
        name="route",
    )(x_in, norm_gain.reshape(1, hidden), w_router, expert_ids, expert_ids.T)


def dispatch(h, ids_t, gates, devices):
    top_k, tokens = ids_t.shape
    table = shape((10, devices, tokens), F32)
    return pl.pallas_call(
        dispatch_kernel,
        out_shape=(table, table) + tuple(shape((devices, SLOTS, w), BF16) for w in WIDTHS),
        in_specs=[VMEM] * 3,
        out_specs=(VMEM, VMEM, ANY, ANY, ANY),
        scratch_shapes=[pltpu.VMEM((3, tokens, w), BF16) for w in WIDTHS]
        + [pltpu.VMEM((9, top_k, tokens), I32), pltpu.VMEM((9, top_k, tokens), F32)]
        + [pltpu.VMEM((devices, SLOTS, w), BF16) for w in WIDTHS]
        + [DMA((3,)), DMA((9,)), DMA, DMA((9,)), DMA, DMA((9,)), DMA((3,)), DMA((3,)), DMA((3, SIDE))],
        compiler_params=params(has_side_effects=True),
        name="dispatch",
    )(h, ids_t, gates)


def experts_mlp(rows, w_gate, w_up, w_down, block):
    devices = rows[0].shape[0]
    blocks = [pltpu.VMEM((devices, SLOTS, w), BF16) for w in WIDTHS]
    return pl.pallas_call(
        functools.partial(expert_kernel, block),
        out_shape=tuple(shape(r.shape, BF16) for r in rows),
        in_specs=[ANY] * 3 + [VMEM] * 3,
        out_specs=(ANY,) * 3,
        scratch_shapes=blocks + blocks + [DMA((3, devices // block)), DMA((3,)), DMA((3,)), DMA((3, SIDE))],
        compiler_params=params(has_side_effects=True),
        name="experts",
    )(*rows, w_gate, w_up, w_down)


def combine(x_in, post, gates, rows):
    tokens, hidden = x_in.shape
    devices = rows[0].shape[0]
    return pl.pallas_call(
        combine_kernel,
        out_shape=shape((tokens, hidden), BF16),
        in_specs=[VMEM] * 3 + [ANY] * 3,
        out_specs=VMEM,
        scratch_shapes=[pltpu.VMEM((devices, SLOTS, w), BF16) for w in WIDTHS]
        + [pltpu.VMEM((SIDE, tokens, w), F32) for w in WIDTHS]
        + [pltpu.VMEM((3, tokens, w), F32) for w in WIDTHS]
        + [DMA((3, SIDE)), DMA((3, 3)), DMA((3, 3))],
        compiler_params=params(has_side_effects=True),
        name="combine",
    )(x_in, post, gates, *rows)


def solution(mesh):
    def local_block(x_in, norm_gain, w_router, expert_ids, w_gate, w_up, w_down):
        h, gates = route(x_in, norm_gain, w_router, expert_ids)
        post, dense, *rows = dispatch(h, expert_ids.T, gates, w_router.shape[1])
        returned = experts_mlp(rows, w_gate, w_up, w_down, 16)
        return combine(x_in, post, dense, returned)

    tok_spec = P(("dp", "ep"), None)
    expert_spec = P("ep", None, None)
    return jax.shard_map(local_block, mesh=mesh, in_specs=(tok_spec, P(None), P(None, None), tok_spec, expert_spec, expert_spec, expert_spec), out_specs=tok_spec, check_vma=False)
```

```python
import functools

import jax
import jax.numpy as jnp
from jax import lax
from jax.experimental import pallas as pl
from jax.experimental.pallas import tpu as pltpu
from jax.sharding import PartitionSpec as P

EPS = 1e-6
SLOTS = 32
SIDE = 4
STRIDES = (2, 8, 32)
WIDTHS = (768, 640, 640)
STARTS = (0, 768, 1408)
PLANE = 32
LAG = 2
F32, BF16, I32 = jnp.float32, jnp.bfloat16, jnp.int32
MESH = pl.DeviceIdType.MESH


def shifted(dev, axis, step):
    stride = STRIDES[axis]
    here = lax.rem(lax.div(dev, stride), SIDE)
    return dev + (lax.rem(here + step, SIDE) - here) * stride


def plane_axes(axis):
    return tuple(a for a in (2, 1, 0) if a != axis)


def in_plane(dev, axis, p):
    a, b = plane_axes(axis)
    dev = shifted(shifted(dev, a, lax.div(p, 8)), b, lax.rem(lax.div(p, 2), SIDE))
    core = lax.rem(dev, 2)
    return dev + lax.rem(core + lax.rem(p, 2), 2) - core


def opposite(p):
    da, db = lax.div(p, 8), lax.rem(lax.div(p, 2), SIDE)
    return lax.rem(SIDE - da, SIDE) * 8 + lax.rem(SIDE - db, SIDE) * 2 + lax.rem(p, 2)


def bit(block, axis):
    return lax.rem(lax.div(block, 1 << axis), 2)


def member(axis, block, m):
    a, b = plane_axes(axis)
    return (bit(block, a) + 2 * lax.div(m, 4)) * 8 + (bit(block, b) + 2 * lax.rem(lax.div(m, 2), 2)) * 2 + lax.rem(m, 2)


def place_of(axis, along, p):
    a, b = plane_axes(axis)
    step = {axis: along, a: lax.div(p, 8), b: lax.rem(lax.div(p, 2), SIDE)}
    odd = (lax.rem(step[2], 2) * 2 + lax.rem(step[1], 2)) * 2 + lax.rem(step[0], 2)
    half = (lax.div(step[2], 2) * 2 + lax.div(step[1], 2)) * 2 + lax.div(step[0], 2)
    return odd * 16 + half * 2 + lax.rem(p, 2)


def split_place(axis, place):
    block, half = lax.div(place, 16), lax.div(lax.rem(place, 16), 2)
    step = tuple(bit(block, i) + 2 * bit(half, i) for i in range(3))
    a, b = plane_axes(axis)
    return step[axis], step[a] * 8 + step[b] * 2 + lax.rem(place, 2)


def remote(src, dst, send_sem, recv_sem, dev):
    return pltpu.make_async_remote_copy(src, dst, send_sem, recv_sem, device_id={"ep": dev}, device_id_type=MESH)


def wait_for(ref, sem):
    pltpu.make_async_copy(ref, ref, sem).wait()


def source(axis, r):
    return 0 if r == 0 else 3 * axis + r


def place_in_tables(axis, r):
    return (3 * axis + r) * lax.min(r, 1)


def route_kernel(x_ref, gain_ref, wr_ref, ids_ref, idst_ref, h_ref, gate_ref):
    tokens, experts = x_ref.shape[0], wr_ref.shape[1]
    top_k = ids_ref.shape[1]
    resid = x_ref[...].astype(F32)
    mean_sq = jnp.mean(resid * resid, axis=-1, keepdims=True)
    normed = (resid * lax.rsqrt(mean_sq + EPS) * gain_ref[...].astype(F32)).astype(BF16)
    h_ref[...] = normed
    logits = jnp.dot(normed, wr_ref[...], preferred_element_type=F32)
    exps = jnp.exp(logits - jnp.max(logits, axis=-1, keepdims=True))
    router_p = exps / jnp.sum(exps, axis=-1, keepdims=True)
    lane_expert = lax.broadcasted_iota(I32, (tokens, experts), 1)
    chosen = jnp.zeros((tokens, experts), F32)
    for j in range(top_k):
        chosen += jnp.where(ids_ref[:, j:j + 1] == lane_expert, 1.0, 0.0)
    picked = router_p * chosen
    gates_t = jnp.transpose(picked / jnp.sum(picked, axis=-1, keepdims=True))
    row_expert = lax.broadcasted_iota(I32, (experts, tokens), 0)
    for j in range(top_k):
        gate_ref[j:j + 1, :] = jnp.sum(jnp.where(idst_ref[j:j + 1, :] == row_expert, gates_t, 0.0), axis=0, keepdims=True)


def dispatch_kernel(h_ref, ids_ref, gate_ref, post_ref, gates_ref, recv0, recv1, recv2,
                    line0, line1, line2, ids_scr, gate_scr, pack0, pack1, pack2,
                    line_send, line_recv, ids_send, ids_recv, gate_send, gate_recv, send_sem, recv_sem, local_sem):
    recv, line, pack = (recv0, recv1, recv2), (line0, line1, line2), (pack0, pack1, pack2)
    top_k, tokens = ids_ref.shape
    experts = post_ref.shape[1]
    me = lax.axis_index("ep")
    for r in (2, 1, 3):
        for axis in range(3):
            dev, k = shifted(me, axis, r), source(axis, SIDE - r)
            n = k - 1
            remote(ids_ref, ids_scr.at[n], ids_send, ids_recv.at[n], dev).start()
            remote(gate_ref, gate_scr.at[n], gate_send, gate_recv.at[n], dev).start()
            cols = h_ref.at[:, pl.ds(STARTS[axis], WIDTHS[axis])]
            remote(cols, line[axis].at[SIDE - r], line_send.at[axis], line_recv.at[n], dev).start()

    row_expert = lax.broadcasted_iota(I32, (experts, tokens), 0)
    rows = lax.broadcasted_iota(I32, (tokens, tokens), 0)
    upper = jnp.where(rows < lax.broadcasted_iota(I32, (tokens, tokens), 1), 1.0, 0.0).astype(BF16)
    slot = lax.broadcasted_iota(I32, (SLOTS, tokens), 0).astype(F32)

    def tables(k, ids, gates):
        chosen = jnp.zeros((experts, tokens), F32)
        dense = jnp.zeros((experts, tokens), F32)
        for j in range(top_k):
            hit = ids[j:j + 1, :] == row_expert
            chosen += jnp.where(hit, 1.0, 0.0)
            dense += jnp.where(hit, gates[j:j + 1, :], 0.0)
        before = jnp.dot(chosen.astype(BF16), upper, preferred_element_type=F32)
        post_ref[k] = jnp.where(chosen > 0.0, before, 255.0)
        gates_ref[k] = dense

    tables(0, ids_ref[...], gate_ref[...])
    for axis in range(3):
        line[axis][0] = h_ref[:, STARTS[axis]:STARTS[axis] + WIDTHS[axis]]

    def arrive(axis, r):
        n = source(axis, r) - 1
        wait_for(ids_scr.at[n], ids_recv.at[n])
        wait_for(gate_scr.at[n], gate_recv.at[n])
        tables(n + 1, ids_scr[n], gate_scr[n])
        wait_for(line[axis].at[r], line_recv.at[n])

    def step(n, carry):
        b, two = lax.div(n, 2), lax.rem(n, 2)
        for axis in range(3):
            @pl.when(n == 1)
            def _():
                arrive(axis, 2)

            @pl.when(n == (2 << axis))
            def _():
                arrive(axis, 1)

            @pl.when(n == (2 << axis) + 1)
            def _():
                arrive(axis, 3)

            r = bit(b, axis) + 2 * two
            k = place_in_tables(axis, r)
            picks = []
            for m in range(8):
                expert = in_plane(me, axis, member(axis, b, m))
                picks.append(jnp.where(post_ref[k, pl.ds(expert, 1), :] == slot, 1.0, 0.0).astype(BF16))
            packed = jnp.dot(jnp.concatenate(picks, axis=0), line[axis][r], preferred_element_type=F32).astype(BF16)
            pack[axis][pl.ds(n * 8, 8)] = packed.reshape(8, SLOTS, WIDTHS[axis])

        def send(m, c):
            for axis in range(3):
                r = bit(b, axis) + 2 * two
                p = member(axis, b, m)
                src = pack[axis].at[n * 8 + m]
                dst = recv[axis].at[place_of(axis, r, opposite(p))]

                @pl.when(p == 0)
                def _():
                    pltpu.make_async_copy(src, dst, local_sem.at[axis, r]).start()

                @pl.when(p != 0)
                def _():
                    remote(src, dst, send_sem.at[axis], recv_sem.at[axis], in_plane(me, axis, p)).start()
            return c

        lax.fori_loop(0, 8, send, 0)
        return carry

    lax.fori_loop(0, 16, step, 0)
    wait_for(ids_scr, ids_send)
    wait_for(gate_scr, gate_send)
    far = SIDE * (PLANE - 1)
    for axis in range(3):
        wait_for(line[axis].at[pl.ds(1, 3)], line_send.at[axis])
        for r in range(SIDE):
            wait_for(recv[axis].at[0], local_sem.at[axis, r])
        wait_for(pack[axis].at[pl.ds(0, far)], send_sem.at[axis])
        wait_for(recv[axis].at[pl.ds(0, far)], recv_sem.at[axis])


def expert_kernel(x_ref, post_ref, gates_ref, x0, x1, x2, wg_ref, wu_ref, wd_ref, out_ref, ret0, ret1, ret2,
                  row0, row1, row2, in0, in1, in2, sum0, sum1, sum2, part0, part1, part2, table_ref,
                  load_sem, back_sem, send_sem, recv_sem, local_sem, line_send, line_recv):
    x, ret, rows, held = (x0, x1, x2), (ret0, ret1, ret2), (row0, row1, row2), (in0, in1, in2)
    sums, parts = (sum0, sum1, sum2), (part0, part1, part2)
    me = lax.axis_index("ep")
    tokens, experts = x_ref.shape[0], post_ref.shape[1]
    blocks, size, width = 8, 16, 8 * SLOTS

    def load(b, axis):
        part = pl.ds(b * size, size)
        return pltpu.make_async_copy(x[axis].at[part], rows[axis].at[part], load_sem.at[axis, b])

    for b in range(blocks):
        for axis in range(3):
            load(b, axis).start()
    for axis in range(3):
        sums[axis][...] = jnp.zeros(sums[axis].shape, F32)

    def mlp(b):
        for axis in range(3):
            load(b, axis).wait()
        gate_val, up_val = 0.0, 0.0
        for axis in range(3):
            part = rows[axis][pl.ds(b * size, size)].reshape(size * SLOTS, WIDTHS[axis])
            span = slice(STARTS[axis], STARTS[axis] + WIDTHS[axis])
            gate_val += jnp.dot(part, wg_ref[0, span, :], preferred_element_type=F32)
            up_val += jnp.dot(part, wu_ref[0, span, :], preferred_element_type=F32)
        act = (jax.nn.silu(gate_val) * up_val).astype(BF16)
        for axis in range(3):
            span = slice(STARTS[axis], STARTS[axis] + WIDTHS[axis])
            y = jnp.dot(act, wd_ref[0, :, span], preferred_element_type=F32).astype(BF16)
            rows[axis][pl.ds(b * size, size)] = y.reshape(size, SLOTS, WIDTHS[axis])

        def send(j, c):
            place = b * size + j
            for axis in range(3):
                along, p = split_place(axis, place)
                src, dst = rows[axis].at[place], ret[axis].at[place]

                @pl.when(p == 0)
                def _():
                    pltpu.make_async_copy(src, dst, local_sem.at[axis, along]).start()

                @pl.when(p != 0)
                def _():
                    remote(src, dst, send_sem.at[axis], recv_sem.at[axis, b], in_plane(me, axis, p)).start()
            return c

        lax.fori_loop(0, size, send, 0)

    def fill_tables(k, c):
        gates = jnp.transpose(gates_ref[k])
        high = gates.astype(BF16)
        rest = gates - high.astype(F32)
        mid = rest.astype(BF16)
        low = (rest - mid.astype(F32)).astype(BF16)
        table_ref[k] = jnp.concatenate([high, mid, low, jnp.transpose(post_ref[k]).astype(BF16)], axis=0)
        return c

    def partial(axis, r):
        return remote(sums[axis].at[r], parts[axis].at[SIDE - r - 1], line_send.at[axis, r - 1], line_recv.at[axis, SIDE - r - 1], shifted(me, axis, r))

    expert = lax.broadcasted_iota(I32, (experts, width), 0)
    column = lax.div(lax.broadcasted_iota(I32, (1, width), 1), SLOTS)
    slot = lax.rem(lax.broadcasted_iota(I32, (1, width), 1), SLOTS).astype(F32)

    def back(b, axis):
        return pltpu.make_async_copy(ret[axis].at[pl.ds(b * size, size)], held[axis], back_sem.at[axis])

    def gather(b):
        for axis in range(3):
            a1, a2 = plane_axes(axis)
            odd = bit(b, axis)
            near = bit(b, a1) + bit(b, a2) == 0

            @pl.when(near)
            def _():
                wait_for(ret[axis].at[0], local_sem.at[axis, odd])
                wait_for(ret[axis].at[0], local_sem.at[axis, odd + 2])
                wait_for(ret[axis].at[pl.ds(0, size - 2)], recv_sem.at[axis, b])

            @pl.when(jnp.logical_not(near))
            def _():
                wait_for(ret[axis].at[pl.ds(0, size)], recv_sem.at[axis, b])

            back(b, axis).start()
        for axis in range(3):
            back(b, axis).wait()
            theirs = in_plane(me, axis, opposite(member(axis, b, column)))
            spread = jnp.where(theirs == expert, 1.0, 0.0).astype(BF16)
            for two in range(2):
                r = bit(b, axis) + 2 * two
                wide = jnp.dot(table_ref[place_in_tables(axis, r)], spread, preferred_element_type=F32)
                hit = wide[3 * tokens:] == slot
                weight = jnp.concatenate([jnp.where(hit, wide[i * tokens:(i + 1) * tokens], 0.0).astype(BF16) for i in range(3)], axis=0)
                run = 2 << axis
                pieces = [held[axis][i:i + run].reshape(run * SLOTS, WIDTHS[axis]) for i in range(two * run, size, 2 * run)]
                got = jnp.dot(weight, jnp.concatenate(pieces, axis=0), preferred_element_type=F32)
                sums[axis][r] += got[:tokens] + got[tokens:2 * tokens] + got[2 * tokens:]
        for axis in range(3):
            @pl.when(b == 7 - (1 << axis))
            def _():
                partial(axis, 2).start()

    def step(t, carry):
        @pl.when(t < blocks)
        def _():
            mlp(t)

        @pl.when(t == LAG - 1)
        def _():
            lax.fori_loop(0, table_ref.shape[0], fill_tables, 0)

        @pl.when(t >= LAG)
        def _():
            gather(t - LAG)
        return carry

    lax.fori_loop(0, blocks + LAG, step, 0)
    for axis in range(3):
        for r in (1, 3):
            partial(axis, r).start()
    for axis in range(3):
        span = slice(STARTS[axis], STARTS[axis] + WIDTHS[axis])
        total = x_ref[:, span].astype(F32) + sums[axis][0]
        for r in (2, 1, 3):
            wait_for(parts[axis].at[r - 1], line_recv.at[axis, r - 1])
            total += parts[axis][r - 1]
        out_ref[:, span] = total.astype(out_ref.dtype)
    far = SIDE * (PLANE - 1)
    for axis in range(3):
        for r in range(1, SIDE):
            wait_for(sums[axis].at[r], line_send.at[axis, r - 1])
        wait_for(rows[axis].at[pl.ds(0, far)], send_sem.at[axis])


def params(**kw):
    return pltpu.CompilerParams(vmem_limit_bytes=62 * 2 ** 20, **kw)


VMEM = pl.BlockSpec(memory_space=pltpu.VMEM)
ANY = pl.BlockSpec(memory_space=pl.ANY)
DMA = pltpu.SemaphoreType.DMA
shape = jax.ShapeDtypeStruct


def route(x_in, norm_gain, w_router, expert_ids):
    tokens, hidden = x_in.shape
    top_k = expert_ids.shape[1]
    return pl.pallas_call(
        route_kernel,
        out_shape=(shape((tokens, hidden), BF16), shape((top_k, tokens), F32)),
        compiler_params=params(),
        name="route",
    )(x_in, norm_gain.reshape(1, hidden), w_router, expert_ids, expert_ids.T)


def dispatch(h, ids_t, gates, devices):
    top_k, tokens = ids_t.shape
    table = shape((10, devices, tokens), F32)
    return pl.pallas_call(
        dispatch_kernel,
        out_shape=(table, table) + tuple(shape((devices, SLOTS, w), BF16) for w in WIDTHS),
        in_specs=[VMEM] * 3,
        out_specs=(VMEM, VMEM, ANY, ANY, ANY),
        scratch_shapes=[pltpu.VMEM((SIDE, tokens, w), BF16) for w in WIDTHS]
        + [pltpu.VMEM((9, top_k, tokens), I32), pltpu.VMEM((9, top_k, tokens), F32)]
        + [pltpu.VMEM((devices, SLOTS, w), BF16) for w in WIDTHS]
        + [DMA((3,)), DMA((9,)), DMA, DMA((9,)), DMA, DMA((9,)), DMA((3,)), DMA((3,)), DMA((3, SIDE))],
        compiler_params=params(has_side_effects=True),
        name="dispatch",
    )(h, ids_t, gates)


def experts_mlp(x_in, post, gates, rows, w_gate, w_up, w_down):
    tokens, hidden = x_in.shape
    devices = rows[0].shape[0]
    out, *_ = pl.pallas_call(
        expert_kernel,
        out_shape=(shape((tokens, hidden), BF16),) + tuple(shape(r.shape, BF16) for r in rows),
        in_specs=[VMEM] * 3 + [ANY] * 3 + [VMEM] * 3,
        out_specs=(VMEM,) + (ANY,) * 3,
        scratch_shapes=[pltpu.VMEM((devices, SLOTS, w), BF16) for w in WIDTHS]
        + [pltpu.VMEM((16, SLOTS, w), BF16) for w in WIDTHS]
        + [pltpu.VMEM((SIDE, tokens, w), F32) for w in WIDTHS]
        + [pltpu.VMEM((3, tokens, w), F32) for w in WIDTHS]
        + [pltpu.VMEM((10, 4 * tokens, devices), BF16)]
        + [DMA((3, 8)), DMA((3,)), DMA((3,)), DMA((3, 8)), DMA((3, SIDE)), DMA((3, 3)), DMA((3, 3))],
        compiler_params=params(has_side_effects=True),
        name="experts",
    )(x_in, post, gates, *rows, w_gate, w_up, w_down)
    return out


def solution(mesh):
    def local_block(x_in, norm_gain, w_router, expert_ids, w_gate, w_up, w_down):
        h, gates = route(x_in, norm_gain, w_router, expert_ids)
        post, dense, *rows = dispatch(h, expert_ids.T, gates, w_router.shape[1])
        return experts_mlp(x_in, post, dense, rows, w_gate, w_up, w_down)

    tok_spec = P(("dp", "ep"), None)
    expert_spec = P("ep", None, None)
    return jax.shard_map(local_block, mesh=mesh, in_specs=(tok_spec, P(None), P(None, None), tok_spec, expert_spec, expert_spec, expert_spec), out_specs=tok_spec, check_vma=False)
```

```python
import functools

import jax
import jax.numpy as jnp
from jax import lax
from jax.experimental import pallas as pl
from jax.experimental.pallas import tpu as pltpu
from jax.sharding import PartitionSpec as P

EPS = 1e-6
SLOTS = 32
SIDE = 4
STRIDES = (2, 8, 32)
WIDTHS = (768, 640, 640)
STARTS = (0, 768, 1408)
PLANE = 32
LAG = 4
F32, BF16, I32 = jnp.float32, jnp.bfloat16, jnp.int32
MESH = pl.DeviceIdType.MESH


def shifted(dev, axis, step):
    stride = STRIDES[axis]
    here = lax.rem(lax.div(dev, stride), SIDE)
    return dev + (lax.rem(here + step, SIDE) - here) * stride


def plane_axes(axis):
    return tuple(a for a in (2, 1, 0) if a != axis)


def in_plane(dev, axis, p):
    a, b = plane_axes(axis)
    dev = shifted(shifted(dev, a, lax.div(p, 8)), b, lax.rem(lax.div(p, 2), SIDE))
    core = lax.rem(dev, 2)
    return dev + lax.rem(core + lax.rem(p, 2), 2) - core


def opposite(p):
    da, db = lax.div(p, 8), lax.rem(lax.div(p, 2), SIDE)
    return lax.rem(SIDE - da, SIDE) * 8 + lax.rem(SIDE - db, SIDE) * 2 + lax.rem(p, 2)


def bit(block, axis):
    return lax.rem(lax.div(block, 1 << axis), 2)


def member(axis, block, m):
    a, b = plane_axes(axis)
    return (bit(block, a) + 2 * lax.div(m, 4)) * 8 + (bit(block, b) + 2 * lax.rem(lax.div(m, 2), 2)) * 2 + lax.rem(m, 2)


def place_of(step, core):
    odd = (lax.rem(step[2], 2) * 2 + lax.rem(step[1], 2)) * 2 + lax.rem(step[0], 2)
    half = (lax.div(step[2], 2) * 2 + lax.div(step[1], 2)) * 2 + lax.div(step[0], 2)
    return odd * 16 + half * 2 + core


def split_place(axis, place):
    block, half = lax.div(place, 16), lax.div(lax.rem(place, 16), 2)
    step = tuple(bit(block, i) + 2 * bit(half, i) for i in range(3))
    a, b = plane_axes(axis)
    return step[axis], step[a] * 8 + step[b] * 2 + lax.rem(place, 2)


def remote(src, dst, send_sem, recv_sem, dev):
    return pltpu.make_async_remote_copy(src, dst, send_sem, recv_sem, device_id={"ep": dev}, device_id_type=MESH)


def wait_for(ref, sem):
    pltpu.make_async_copy(ref, ref, sem).wait()


def source(axis, r):
    return 0 if r == 0 else 3 * axis + r


def place_in_tables(axis, r):
    return (3 * axis + r) * lax.min(r, 1)


def route_kernel(x_ref, gain_ref, wr_ref, ids_ref, idst_ref, h_ref, gate_ref):
    tokens, experts = x_ref.shape[0], wr_ref.shape[1]
    top_k = ids_ref.shape[1]
    resid = x_ref[...].astype(F32)
    mean_sq = jnp.mean(resid * resid, axis=-1, keepdims=True)
    normed = (resid * lax.rsqrt(mean_sq + EPS) * gain_ref[...].astype(F32)).astype(BF16)
    h_ref[...] = normed
    logits = jnp.dot(normed, wr_ref[...], preferred_element_type=F32)
    exps = jnp.exp(logits - jnp.max(logits, axis=-1, keepdims=True))
    router_p = exps / jnp.sum(exps, axis=-1, keepdims=True)
    lane_expert = lax.broadcasted_iota(I32, (tokens, experts), 1)
    chosen = jnp.zeros((tokens, experts), F32)
    for j in range(top_k):
        chosen += jnp.where(ids_ref[:, j:j + 1] == lane_expert, 1.0, 0.0)
    picked = router_p * chosen
    gates_t = jnp.transpose(picked / jnp.sum(picked, axis=-1, keepdims=True))
    row_expert = lax.broadcasted_iota(I32, (experts, tokens), 0)
    for j in range(top_k):
        gate_ref[j:j + 1, :] = jnp.sum(jnp.where(idst_ref[j:j + 1, :] == row_expert, gates_t, 0.0), axis=0, keepdims=True)


def dispatch_kernel(h_ref, ids_ref, gate_ref, post_ref, gates_ref, recv0, recv1, recv2,
                    line0, line1, line2, ids_scr, gate_scr, pack0, pack1, pack2,
                    line_send, line_recv, ids_send, ids_recv, gate_send, gate_recv, send_sem, recv_sem, local_sem):
    recv, line, pack = (recv0, recv1, recv2), (line0, line1, line2), (pack0, pack1, pack2)
    top_k, tokens = ids_ref.shape
    experts = post_ref.shape[1]
    me = lax.axis_index("ep")

    def forward(axis, r, src):
        for q in (2, 1, 3):
            n = r * SIDE + SIDE - q
            remote(src, line[axis].at[n], line_send.at[axis], line_recv.at[axis, n], shifted(me, (axis + 1) % 3, q)).start()

    for axis in range(3):
        for n in range(1, SIDE * SIDE):
            r, q = n // SIDE, n % SIDE
            dev = shifted(shifted(me, axis, r), (axis + 1) % 3, q)
            there = ((SIDE - r) % SIDE) * SIDE + (SIDE - q) % SIDE
            remote(ids_ref, ids_scr.at[axis, there], ids_send.at[axis], ids_recv.at[axis], dev).start()
    for r in (2, 1, 3):
        for axis in range(3):
            n = (SIDE - r) * SIDE
            src = h_ref.at[:, pl.ds(STARTS[axis], WIDTHS[axis])]
            remote(src, line[axis].at[n], line_send.at[axis], line_recv.at[axis, n], shifted(me, axis, r)).start()
    for axis in range(3):
        forward(axis, 0, h_ref.at[:, pl.ds(STARTS[axis], WIDTHS[axis])])
    for axis in range(3):
        for r in range(1, SIDE):
            k = 3 * axis + SIDE - r - 1
            remote(gate_ref, gate_scr.at[k], gate_send, gate_recv, shifted(me, axis, r)).start()
        line[axis][0] = h_ref[:, STARTS[axis]:STARTS[axis] + WIDTHS[axis]]
        ids_scr[axis, 0] = ids_ref[...]

    row_expert = lax.broadcasted_iota(I32, (experts, tokens), 0)
    rows = lax.broadcasted_iota(I32, (tokens, tokens), 0)
    upper = jnp.where(rows < lax.broadcasted_iota(I32, (tokens, tokens), 1), 1.0, 0.0).astype(BF16)
    slot = lax.broadcasted_iota(I32, (8, SLOTS, tokens), 1).astype(F32)
    eight = lax.broadcasted_iota(I32, (8, tokens), 0)

    def across(axis, m):
        dev = shifted(me, (axis + 2) % 3, lax.div(m, 2))
        core = lax.rem(dev, 2)
        return dev + lax.rem(core + lax.rem(m, 2), 2) - core

    def swap(v):
        return v + lax.div(v, 2) * (5 - 2 * v)

    def step(t, carry):
        r, q = swap(lax.rem(t, SIDE)), swap(lax.div(t, SIDE))
        n = r * SIDE + q
        for axis in range(3):
            @pl.when(t == 1)
            def _():
                wait_for(ids_scr.at[axis, pl.ds(1, SIDE * SIDE - 1)], ids_recv.at[axis])

            @pl.when(t > 0)
            def _():
                wait_for(line[axis].at[n], line_recv.at[axis, n])

            @pl.when((t > 0) & (t < SIDE))
            def _():
                forward(axis, r, line[axis].at[n])

            theirs = across(axis, eight)
            chosen = jnp.zeros((8, tokens), F32)
            for j in range(top_k):
                chosen += jnp.where(ids_scr[axis, n, j:j + 1, :] == theirs, 1.0, 0.0)
            before = jnp.dot(chosen.astype(BF16), upper, preferred_element_type=F32)
            post = jnp.where(chosen > 0.0, before, 255.0)
            pick = jnp.where(post[:, None, :] == slot, 1.0, 0.0).astype(BF16).reshape(8 * SLOTS, tokens)
            packed = jnp.dot(pick, line[axis][n], preferred_element_type=F32).astype(BF16)
            pack[axis][pl.ds(t * 8, 8)] = packed.reshape(8, SLOTS, WIDTHS[axis])

        def send(i, c):
            m = lax.rem(i + 2, 8)
            for axis in range(3):
                steps = {axis: r, (axis + 1) % 3: q, (axis + 2) % 3: lax.rem(SIDE - lax.div(m, 2), SIDE)}
                src = pack[axis].at[t * 8 + m]
                dst = recv[axis].at[place_of(steps, lax.rem(m, 2))]

                @pl.when(m == 0)
                def _():
                    pltpu.make_async_copy(src, dst, local_sem.at[axis, t]).start()

                @pl.when(m != 0)
                def _():
                    remote(src, dst, send_sem.at[axis], recv_sem.at[axis], across(axis, m)).start()
            return c

        lax.fori_loop(0, 8, send, 0)
        return carry

    steps = SIDE * SIDE
    lax.fori_loop(0, steps, step, 0)

    def tables(k, ids, gates):
        chosen = jnp.zeros((experts, tokens), F32)
        dense = jnp.zeros((experts, tokens), F32)
        for j in range(top_k):
            hit = ids[j:j + 1, :] == row_expert
            chosen += jnp.where(hit, 1.0, 0.0)
            dense += jnp.where(hit, gates[j:j + 1, :], 0.0)
        before = jnp.dot(chosen.astype(BF16), upper, preferred_element_type=F32)
        post_ref[k] = jnp.where(chosen > 0.0, before, 255.0)
        gates_ref[k] = dense

    wait_for(gate_scr, gate_recv)
    tables(0, ids_ref[...], gate_ref[...])
    for axis in range(3):
        for r in range(1, SIDE):
            k = source(axis, r)
            tables(k, ids_scr[axis, r * SIDE], gate_scr[k - 1])

    wait_for(gate_scr, gate_send)
    for axis in range(3):
        wait_for(ids_scr.at[axis, pl.ds(1, steps - 1)], ids_send.at[axis])
        wait_for(line[axis].at[pl.ds(1, steps - 1)], line_send.at[axis])
        for t in range(steps):
            wait_for(recv[axis].at[0], local_sem.at[axis, t])
        wait_for(pack[axis].at[pl.ds(0, 7 * steps)], send_sem.at[axis])
        wait_for(recv[axis].at[pl.ds(0, 7 * steps)], recv_sem.at[axis])


def expert_kernel(x_ref, post_ref, gates_ref, x0, x1, x2, wg_ref, wu_ref, wd_ref, out_ref, ret0, ret1, ret2,
                  row0, row1, row2, in0, in1, in2, sum0, sum1, sum2, part0, part1, part2, table_ref,
                  load_sem, back_sem, send_sem, recv_sem, local_sem, line_send, line_recv):
    x, ret, rows, held = (x0, x1, x2), (ret0, ret1, ret2), (row0, row1, row2), (in0, in1, in2)
    sums, parts = (sum0, sum1, sum2), (part0, part1, part2)
    me = lax.axis_index("ep")
    tokens, experts = x_ref.shape[0], post_ref.shape[1]
    blocks, size, width = 8, 16, 8 * SLOTS

    def load(b, axis):
        part = pl.ds(b * size, size)
        return pltpu.make_async_copy(x[axis].at[part], rows[axis].at[part], load_sem.at[axis, b])

    for b in range(blocks):
        for axis in range(3):
            load(b, axis).start()
    for axis in range(3):
        sums[axis][...] = jnp.zeros(sums[axis].shape, F32)

    def mlp(b):
        for axis in range(3):
            load(b, axis).wait()
        gate_val, up_val = 0.0, 0.0
        for axis in range(3):
            part = rows[axis][pl.ds(b * size, size)].reshape(size * SLOTS, WIDTHS[axis])
            span = slice(STARTS[axis], STARTS[axis] + WIDTHS[axis])
            gate_val += jnp.dot(part, wg_ref[0, span, :], preferred_element_type=F32)
            up_val += jnp.dot(part, wu_ref[0, span, :], preferred_element_type=F32)
        act = (jax.nn.silu(gate_val) * up_val).astype(BF16)
        for axis in range(3):
            span = slice(STARTS[axis], STARTS[axis] + WIDTHS[axis])
            y = jnp.dot(act, wd_ref[0, :, span], preferred_element_type=F32).astype(BF16)
            rows[axis][pl.ds(b * size, size)] = y.reshape(size, SLOTS, WIDTHS[axis])

        def send(j, c):
            place = b * size + j
            for axis in range(3):
                along, p = split_place(axis, place)
                src, dst = rows[axis].at[place], ret[axis].at[place]

                @pl.when(p == 0)
                def _():
                    pltpu.make_async_copy(src, dst, local_sem.at[axis, along]).start()

                @pl.when(p != 0)
                def _():
                    remote(src, dst, send_sem.at[axis], recv_sem.at[axis, b], in_plane(me, axis, p)).start()
            return c

        lax.fori_loop(0, size, send, 0)

    def fill_tables(k, c):
        gates = jnp.transpose(gates_ref[k])
        high = gates.astype(BF16)
        rest = gates - high.astype(F32)
        mid = rest.astype(BF16)
        low = (rest - mid.astype(F32)).astype(BF16)
        table_ref[k] = jnp.concatenate([high, mid, low, jnp.transpose(post_ref[k]).astype(BF16)], axis=0)
        return c

    def partial(axis, r):
        return remote(sums[axis].at[r], parts[axis].at[SIDE - r - 1], line_send.at[axis, r - 1], line_recv.at[axis, SIDE - r - 1], shifted(me, axis, r))

    expert = lax.broadcasted_iota(I32, (experts, width), 0)
    column = lax.div(lax.broadcasted_iota(I32, (1, width), 1), SLOTS)
    slot = lax.rem(lax.broadcasted_iota(I32, (1, width), 1), SLOTS).astype(F32)

    def back(b, axis):
        return pltpu.make_async_copy(ret[axis].at[pl.ds(b * size, size)], held[axis], back_sem.at[axis])

    def gather(b):
        for axis in range(3):
            a1, a2 = plane_axes(axis)
            odd = bit(b, axis)
            near = bit(b, a1) + bit(b, a2) == 0

            @pl.when(near)
            def _():
                wait_for(ret[axis].at[0], local_sem.at[axis, odd])
                wait_for(ret[axis].at[0], local_sem.at[axis, odd + 2])
                wait_for(ret[axis].at[pl.ds(0, size - 2)], recv_sem.at[axis, b])

            @pl.when(jnp.logical_not(near))
            def _():
                wait_for(ret[axis].at[pl.ds(0, size)], recv_sem.at[axis, b])

            back(b, axis).start()
        for axis in range(3):
            back(b, axis).wait()
            theirs = in_plane(me, axis, opposite(member(axis, b, column)))
            spread = jnp.where(theirs == expert, 1.0, 0.0).astype(BF16)
            for two in range(2):
                r = bit(b, axis) + 2 * two
                wide = jnp.dot(table_ref[place_in_tables(axis, r)], spread, preferred_element_type=F32)
                hit = wide[3 * tokens:] == slot
                weight = jnp.concatenate([jnp.where(hit, wide[i * tokens:(i + 1) * tokens], 0.0).astype(BF16) for i in range(3)], axis=0)
                run = 2 << axis
                pieces = [held[axis][i:i + run].reshape(run * SLOTS, WIDTHS[axis]) for i in range(two * run, size, 2 * run)]
                got = jnp.dot(weight, jnp.concatenate(pieces, axis=0), preferred_element_type=F32)
                sums[axis][r] += got[:tokens] + got[tokens:2 * tokens] + got[2 * tokens:]
        for axis in range(3):
            @pl.when(b == 7 - (1 << axis))
            def _():
                partial(axis, 2).start()

    def step(t, carry):
        @pl.when(t < blocks)
        def _():
            mlp(t)

        @pl.when(t == LAG - 1)
        def _():
            lax.fori_loop(0, table_ref.shape[0], fill_tables, 0)

        @pl.when(t >= LAG)
        def _():
            gather(t - LAG)
        return carry

    lax.fori_loop(0, blocks + LAG, step, 0)
    for axis in range(3):
        for r in (1, 3):
            partial(axis, r).start()
    for axis in range(3):
        span = slice(STARTS[axis], STARTS[axis] + WIDTHS[axis])
        total = x_ref[:, span].astype(F32) + sums[axis][0]
        for r in (2, 1, 3):
            wait_for(parts[axis].at[r - 1], line_recv.at[axis, r - 1])
            total += parts[axis][r - 1]
        out_ref[:, span] = total.astype(out_ref.dtype)
    far = SIDE * (PLANE - 1)
    for axis in range(3):
        for r in range(1, SIDE):
            wait_for(sums[axis].at[r], line_send.at[axis, r - 1])
        wait_for(rows[axis].at[pl.ds(0, far)], send_sem.at[axis])


def params(**kw):
    return pltpu.CompilerParams(vmem_limit_bytes=62 * 2 ** 20, **kw)


VMEM = pl.BlockSpec(memory_space=pltpu.VMEM)
ANY = pl.BlockSpec(memory_space=pl.ANY)
DMA = pltpu.SemaphoreType.DMA
shape = jax.ShapeDtypeStruct


def route(x_in, norm_gain, w_router, expert_ids):
    tokens, hidden = x_in.shape
    top_k = expert_ids.shape[1]
    return pl.pallas_call(
        route_kernel,
        out_shape=(shape((tokens, hidden), BF16), shape((top_k, tokens), F32)),
        compiler_params=params(),
        name="route",
    )(x_in, norm_gain.reshape(1, hidden), w_router, expert_ids, expert_ids.T)


def dispatch(h, ids_t, gates, devices):
    top_k, tokens = ids_t.shape
    table = shape((10, devices, tokens), F32)
    return pl.pallas_call(
        dispatch_kernel,
        out_shape=(table, table) + tuple(shape((devices, SLOTS, w), BF16) for w in WIDTHS),
        in_specs=[VMEM] * 3,
        out_specs=(VMEM, VMEM, ANY, ANY, ANY),
        scratch_shapes=[pltpu.VMEM((SIDE * SIDE, tokens, w), BF16) for w in WIDTHS]
        + [pltpu.VMEM((3, SIDE * SIDE, top_k, tokens), I32), pltpu.VMEM((9, top_k, tokens), F32)]
        + [pltpu.VMEM((devices, SLOTS, w), BF16) for w in WIDTHS]
        + [DMA((3,)), DMA((3, SIDE * SIDE)), DMA((3,)), DMA((3,)), DMA, DMA, DMA((3,)), DMA((3,)), DMA((3, SIDE * SIDE))],
        compiler_params=params(has_side_effects=True),
        name="dispatch",
    )(h, ids_t, gates)


def experts_mlp(x_in, post, gates, rows, w_gate, w_up, w_down):
    tokens, hidden = x_in.shape
    devices = rows[0].shape[0]
    out, *_ = pl.pallas_call(
        expert_kernel,
        out_shape=(shape((tokens, hidden), BF16),) + tuple(shape(r.shape, BF16) for r in rows),
        in_specs=[VMEM] * 3 + [ANY] * 3 + [VMEM] * 3,
        out_specs=(VMEM,) + (ANY,) * 3,
        scratch_shapes=[pltpu.VMEM((devices, SLOTS, w), BF16) for w in WIDTHS]
        + [pltpu.VMEM((16, SLOTS, w), BF16) for w in WIDTHS]
        + [pltpu.VMEM((SIDE, tokens, w), F32) for w in WIDTHS]
        + [pltpu.VMEM((3, tokens, w), F32) for w in WIDTHS]
        + [pltpu.VMEM((10, 4 * tokens, devices), BF16)]
        + [DMA((3, 8)), DMA((3,)), DMA((3,)), DMA((3, 8)), DMA((3, SIDE)), DMA((3, 3)), DMA((3, 3))],
        compiler_params=params(has_side_effects=True),
        name="experts",
    )(x_in, post, gates, *rows, w_gate, w_up, w_down)
    return out


def solution(mesh):
    def local_block(x_in, norm_gain, w_router, expert_ids, w_gate, w_up, w_down):
        h, gates = route(x_in, norm_gain, w_router, expert_ids)
        post, dense, *rows = dispatch(h, expert_ids.T, gates, w_router.shape[1])
        return experts_mlp(x_in, post, dense, rows, w_gate, w_up, w_down)

    tok_spec = P(("dp", "ep"), None)
    expert_spec = P("ep", None, None)
    return jax.shard_map(local_block, mesh=mesh, in_specs=(tok_spec, P(None), P(None, None), tok_spec, expert_spec, expert_spec, expert_spec), out_specs=tok_spec, check_vma=False)
```

```python
import functools

import jax
import jax.numpy as jnp
from jax import lax
from jax.experimental import pallas as pl
from jax.experimental.pallas import tpu as pltpu
from jax.sharding import PartitionSpec as P

EPS = 1e-6
SLOTS = 32
SIDE = 4
STRIDES = (2, 8, 32)
WIDTHS = (768, 640, 640)
STARTS = (0, 768, 1408)
CUT = 384
PLANE = 32
LAG = 7
F32, BF16, I32 = jnp.float32, jnp.bfloat16, jnp.int32
MESH = pl.DeviceIdType.MESH


def shifted(dev, axis, step):
    stride = STRIDES[axis]
    here = lax.rem(lax.div(dev, stride), SIDE)
    return dev + (lax.rem(here + step, SIDE) - here) * stride


def plane_axes(axis):
    return tuple(a for a in (2, 1, 0) if a != axis)


def in_plane(dev, axis, p):
    a, b = plane_axes(axis)
    dev = shifted(shifted(dev, a, lax.div(p, 8)), b, lax.rem(lax.div(p, 2), SIDE))
    core = lax.rem(dev, 2)
    return dev + lax.rem(core + lax.rem(p, 2), 2) - core


def opposite(p):
    da, db = lax.div(p, 8), lax.rem(lax.div(p, 2), SIDE)
    return lax.rem(SIDE - da, SIDE) * 8 + lax.rem(SIDE - db, SIDE) * 2 + lax.rem(p, 2)


def bit(block, axis):
    return lax.rem(lax.div(block, 1 << axis), 2)


def member(axis, block, m):
    a, b = plane_axes(axis)
    return (bit(block, a) + 2 * lax.div(m, 4)) * 8 + (bit(block, b) + 2 * lax.rem(lax.div(m, 2), 2)) * 2 + lax.rem(m, 2)


def place_of(step, core):
    odd = (lax.rem(step[2], 2) * 2 + lax.rem(step[1], 2)) * 2 + lax.rem(step[0], 2)
    half = (lax.div(step[2], 2) * 2 + lax.div(step[1], 2)) * 2 + lax.div(step[0], 2)
    return odd * 16 + half * 2 + core


def split_place(axis, place):
    block, half = lax.div(place, 16), lax.div(lax.rem(place, 16), 2)
    step = tuple(bit(block, i) + 2 * bit(half, i) for i in range(3))
    a, b = plane_axes(axis)
    return step[axis], step[a] * 8 + step[b] * 2 + lax.rem(place, 2)


def remote(src, dst, send_sem, recv_sem, dev):
    return pltpu.make_async_remote_copy(src, dst, send_sem, recv_sem, device_id={"ep": dev}, device_id_type=MESH)


def wait_for(ref, sem):
    pltpu.make_async_copy(ref, ref, sem).wait()


def source(axis, r):
    return 0 if r == 0 else 3 * axis + r


def place_in_tables(axis, r):
    return (3 * axis + r) * lax.min(r, 1)


def route_kernel(x_ref, gain_ref, wr_ref, ids_ref, idst_ref, h_ref, gate_ref):
    tokens, experts = x_ref.shape[0], wr_ref.shape[1]
    top_k = ids_ref.shape[1]
    resid = x_ref[...].astype(F32)
    mean_sq = jnp.mean(resid * resid, axis=-1, keepdims=True)
    normed = (resid * lax.rsqrt(mean_sq + EPS) * gain_ref[...].astype(F32)).astype(BF16)
    h_ref[...] = normed
    logits = jnp.dot(normed, wr_ref[...], preferred_element_type=F32)
    exps = jnp.exp(logits - jnp.max(logits, axis=-1, keepdims=True))
    router_p = exps / jnp.sum(exps, axis=-1, keepdims=True)
    lane_expert = lax.broadcasted_iota(I32, (tokens, experts), 1)
    chosen = jnp.zeros((tokens, experts), F32)
    for j in range(top_k):
        chosen += jnp.where(ids_ref[:, j:j + 1] == lane_expert, 1.0, 0.0)
    picked = router_p * chosen
    gates_t = jnp.transpose(picked / jnp.sum(picked, axis=-1, keepdims=True))
    row_expert = lax.broadcasted_iota(I32, (experts, tokens), 0)
    for j in range(top_k):
        gate_ref[j:j + 1, :] = jnp.sum(jnp.where(idst_ref[j:j + 1, :] == row_expert, gates_t, 0.0), axis=0, keepdims=True)


def dispatch_kernel(h_ref, ids_ref, gate_ref, post_ref, gates_ref, recv0, recv1, recv2,
                    line0, line1, line2, ids_scr, gate_scr, pack0, pack1, pack2,
                    line_send, line_recv, ids_send, ids_recv, gate_send, gate_recv, send_sem, recv_sem, local_sem):
    recv, line, pack = (recv0, recv1, recv2), (line0, line1, line2), (pack0, pack1, pack2)
    top_k, tokens = ids_ref.shape
    experts = post_ref.shape[1]
    me = lax.axis_index("ep")

    def forward(axis, r, src):
        for q in (1, 3):
            n = r * SIDE + SIDE - q
            remote(src, line[axis].at[n], line_send.at[axis], line_recv.at[axis, n], shifted(me, (axis + 1) % 3, q)).start()

    def pass_on(axis, r, q, first):
        part, n = pl.ds(first, tokens // 2), r * SIDE + 2
        remote(line[axis].at[r * SIDE + q, part], line[axis].at[n, part], line_send.at[axis], line_recv.at[axis, n], shifted(me, (axis + 1) % 3, SIDE - q)).start()

    for axis in range(3):
        for n in range(1, SIDE * SIDE):
            r, q = n // SIDE, n % SIDE
            dev = shifted(shifted(me, axis, r), (axis + 1) % 3, q)
            there = ((SIDE - r) % SIDE) * SIDE + (SIDE - q) % SIDE
            remote(ids_ref, ids_scr.at[axis, there], ids_send.at[axis], ids_recv.at[axis], dev).start()
    for r in (2, 1, 3):
        for axis in range(3):
            n = (SIDE - r) * SIDE
            src = h_ref.at[:, pl.ds(STARTS[axis], WIDTHS[axis])]
            remote(src, line[axis].at[n], line_send.at[axis], line_recv.at[axis, n], shifted(me, axis, r)).start()
    for axis in range(3):
        forward(axis, 0, h_ref.at[:, pl.ds(STARTS[axis], WIDTHS[axis])])
    for axis in range(3):
        for r in range(1, SIDE):
            k = 3 * axis + SIDE - r - 1
            remote(gate_ref, gate_scr.at[k], gate_send, gate_recv, shifted(me, axis, r)).start()
        line[axis][0] = h_ref[:, STARTS[axis]:STARTS[axis] + WIDTHS[axis]]
        ids_scr[axis, 0] = ids_ref[...]

    row_expert = lax.broadcasted_iota(I32, (experts, tokens), 0)
    rows = lax.broadcasted_iota(I32, (tokens, tokens), 0)
    upper = jnp.where(rows < lax.broadcasted_iota(I32, (tokens, tokens), 1), 1.0, 0.0).astype(BF16)
    slot = lax.broadcasted_iota(I32, (8, SLOTS, tokens), 1).astype(F32)
    eight = lax.broadcasted_iota(I32, (8, tokens), 0)

    def across(axis, m):
        dev = shifted(me, (axis + 2) % 3, lax.div(m, 2))
        core = lax.rem(dev, 2)
        return dev + lax.rem(core + lax.rem(m, 2), 2) - core

    def swap(v):
        return v + lax.div(v, 2) * (5 - 2 * v)

    def step(t, carry):
        r, q = swap(lax.rem(t, SIDE)), swap(lax.div(t, SIDE))
        n = r * SIDE + q
        for axis in range(3):
            @pl.when(t == 1)
            def _():
                wait_for(ids_scr.at[axis, pl.ds(1, SIDE * SIDE - 1)], ids_recv.at[axis])

            @pl.when(t > 0)
            def _():
                wait_for(line[axis].at[n], line_recv.at[axis, n])

            @pl.when((t > 0) & (t < SIDE))
            def _():
                forward(axis, r, line[axis].at[n])

            @pl.when((t >= SIDE) & (t < 2 * SIDE))
            def _():
                pass_on(axis, r, 1, tokens // 2)

            @pl.when((t >= 2 * SIDE) & (t < 3 * SIDE))
            def _():
                pass_on(axis, r, 3, 0)

            theirs = across(axis, eight)
            chosen = jnp.zeros((8, tokens), F32)
            for j in range(top_k):
                chosen += jnp.where(ids_scr[axis, n, j:j + 1, :] == theirs, 1.0, 0.0)
            before = jnp.dot(chosen.astype(BF16), upper, preferred_element_type=F32)
            post = jnp.where(chosen > 0.0, before, 255.0)
            pick = jnp.where(post[:, None, :] == slot, 1.0, 0.0).astype(BF16).reshape(8 * SLOTS, tokens)
            packed = jnp.dot(pick, line[axis][n], preferred_element_type=F32).astype(BF16)
            pack[axis][pl.ds(t * 8, 8)] = packed.reshape(8, SLOTS, WIDTHS[axis])

        def send(i, c):
            m = lax.rem(i + 2, 8)
            for axis in range(3):
                steps = {axis: r, (axis + 1) % 3: q, (axis + 2) % 3: lax.rem(SIDE - lax.div(m, 2), SIDE)}
                src = pack[axis].at[t * 8 + m]
                dst = recv[axis].at[place_of(steps, lax.rem(m, 2))]

                @pl.when(m == 0)
                def _():
                    pltpu.make_async_copy(src, dst, local_sem.at[axis, t]).start()

                @pl.when(m != 0)
                def _():
                    remote(src, dst, send_sem.at[axis], recv_sem.at[axis], across(axis, m)).start()
            return c

        lax.fori_loop(0, 8, send, 0)
        return carry

    steps = SIDE * SIDE
    lax.fori_loop(0, steps, step, 0)

    def tables(k, ids, gates):
        chosen = jnp.zeros((experts, tokens), F32)
        dense = jnp.zeros((experts, tokens), F32)
        for j in range(top_k):
            hit = ids[j:j + 1, :] == row_expert
            chosen += jnp.where(hit, 1.0, 0.0)
            dense += jnp.where(hit, gates[j:j + 1, :], 0.0)
        before = jnp.dot(chosen.astype(BF16), upper, preferred_element_type=F32)
        post_ref[k] = jnp.where(chosen > 0.0, before, 255.0)
        gates_ref[k] = dense

    wait_for(gate_scr, gate_recv)
    tables(0, ids_ref[...], gate_ref[...])
    for axis in range(3):
        for r in range(1, SIDE):
            k = source(axis, r)
            tables(k, ids_scr[axis, r * SIDE], gate_scr[k - 1])

    wait_for(gate_scr, gate_send)
    for axis in range(3):
        wait_for(ids_scr.at[axis, pl.ds(1, steps - 1)], ids_send.at[axis])
        wait_for(line[axis].at[pl.ds(1, steps - 1)], line_send.at[axis])
        for t in range(steps):
            wait_for(recv[axis].at[0], local_sem.at[axis, t])
        wait_for(pack[axis].at[pl.ds(0, 7 * steps)], send_sem.at[axis])
        wait_for(recv[axis].at[pl.ds(0, 7 * steps)], recv_sem.at[axis])


def expert_kernel(x_ref, post_ref, gates_ref, x0, x1, x2, wg_ref, wu_ref, wd_ref, out_ref, ret0, ret1, ret2,
                  row0, row1, row2, in0, in1, in2, sum0, sum1, sum2, part0, part1, part2, act_ref, table_ref,
                  load_sem, back_sem, send_sem, recv_sem, local_sem, line_send, line_recv):
    x, ret, rows, held = (x0, x1, x2), (ret0, ret1, ret2), (row0, row1, row2), (in0, in1, in2)
    sums, parts = (sum0, sum1, sum2), (part0, part1, part2)
    me = lax.axis_index("ep")
    tokens, experts = x_ref.shape[0], post_ref.shape[1]
    blocks, size, width = 8, 16, 8 * SLOTS
    spans = [[pl.ds(0, CUT) for w in WIDTHS], [pl.ds(CUT, w - CUT) for w in WIDTHS]]

    def load(b, axis):
        part = pl.ds(b * size, size)
        return pltpu.make_async_copy(x[axis].at[part], rows[axis].at[part], load_sem.at[axis, b])

    for b in range(blocks):
        for axis in range(3):
            load(b, axis).start()
    for axis in range(3):
        sums[axis][...] = jnp.zeros(sums[axis].shape, F32)

    def activate(b):
        for axis in range(3):
            load(b, axis).wait()
        gate_val, up_val = 0.0, 0.0
        for axis in range(3):
            part = rows[axis][pl.ds(b * size, size)].reshape(size * SLOTS, WIDTHS[axis])
            span = slice(STARTS[axis], STARTS[axis] + WIDTHS[axis])
            gate_val += jnp.dot(part, wg_ref[0, span, :], preferred_element_type=F32)
            up_val += jnp.dot(part, wu_ref[0, span, :], preferred_element_type=F32)
        act_ref[b] = (jax.nn.silu(gate_val) * up_val).astype(BF16)

    def project(b, turn):
        for axis in range(3):
            span = spans[turn][axis]
            y = jnp.dot(act_ref[b], wd_ref[0, :, pl.ds(STARTS[axis] + span.start, span.size)], preferred_element_type=F32).astype(BF16)
            rows[axis][pl.ds(b * size, size), :, span] = y.reshape(size, SLOTS, span.size)

        def send(j, c):
            place = b * size + j
            for axis in range(3):
                along, p = split_place(axis, place)
                src, dst = rows[axis].at[place, :, spans[turn][axis]], ret[axis].at[place, :, spans[turn][axis]]

                @pl.when(p == 0)
                def _():
                    pltpu.make_async_copy(src, dst, local_sem.at[axis, turn * SIDE + along]).start()

                @pl.when(p != 0)
                def _():
                    remote(src, dst, send_sem.at[axis, turn], recv_sem.at[axis, turn * blocks + b], in_plane(me, axis, p)).start()
            return c

        lax.fori_loop(0, size, send, 0)

    def fill_tables(k, c):
        gates = jnp.transpose(gates_ref[k])
        high = gates.astype(BF16)
        rest = gates - high.astype(F32)
        mid = rest.astype(BF16)
        low = (rest - mid.astype(F32)).astype(BF16)
        table_ref[k] = jnp.concatenate([high, mid, low, jnp.transpose(post_ref[k]).astype(BF16)], axis=0)
        return c

    def partial(axis, r, turn):
        span = spans[turn][axis]
        return remote(sums[axis].at[r, :, span], parts[axis].at[SIDE - r - 1, :, span], line_send.at[axis, turn * 3 + r - 1], line_recv.at[axis, turn * 3 + SIDE - r - 1], shifted(me, axis, r))

    expert = lax.broadcasted_iota(I32, (experts, width), 0)
    column = lax.div(lax.broadcasted_iota(I32, (1, width), 1), SLOTS)
    slot = lax.rem(lax.broadcasted_iota(I32, (1, width), 1), SLOTS).astype(F32)

    def gather(b, turn):
        def back(axis):
            span = spans[turn][axis]
            return pltpu.make_async_copy(ret[axis].at[pl.ds(b * size, size), :, span], held[axis].at[:, :, span], back_sem.at[axis])

        for axis in range(3):
            a1, a2 = plane_axes(axis)
            odd, span = bit(b, axis), spans[turn][axis]
            near = bit(b, a1) + bit(b, a2) == 0

            @pl.when(near)
            def _():
                wait_for(ret[axis].at[0, :, span], local_sem.at[axis, turn * SIDE + odd])
                wait_for(ret[axis].at[0, :, span], local_sem.at[axis, turn * SIDE + odd + 2])
                wait_for(ret[axis].at[pl.ds(0, size - 2), :, span], recv_sem.at[axis, turn * blocks + b])

            @pl.when(jnp.logical_not(near))
            def _():
                wait_for(ret[axis].at[pl.ds(0, size), :, span], recv_sem.at[axis, turn * blocks + b])

            back(axis).start()
        for axis in range(3):
            span = spans[turn][axis]
            back(axis).wait()
            theirs = in_plane(me, axis, opposite(member(axis, b, column)))
            spread = jnp.where(theirs == expert, 1.0, 0.0).astype(BF16)
            for two in range(2):
                r = bit(b, axis) + 2 * two
                wide = jnp.dot(table_ref[place_in_tables(axis, r)], spread, preferred_element_type=F32)
                hit = wide[3 * tokens:] == slot
                weight = jnp.concatenate([jnp.where(hit, wide[i * tokens:(i + 1) * tokens], 0.0).astype(BF16) for i in range(3)], axis=0)
                run = 2 << axis
                pieces = [held[axis][i:i + run, :, span].reshape(run * SLOTS, span.size) for i in range(two * run, size, 2 * run)]
                got = jnp.dot(weight, jnp.concatenate(pieces, axis=0), preferred_element_type=F32)
                sums[axis][r, :, span] += got[:tokens] + got[tokens:2 * tokens] + got[2 * tokens:]
        for axis in range(3):
            @pl.when(b == 7 - (1 << axis))
            def _():
                partial(axis, 2, turn).start()

            @pl.when(b == 7)
            def _():
                partial(axis, 1, turn).start()
                partial(axis, 3, turn).start()

    def step(t, carry):
        @pl.when(t < blocks)
        def _():
            activate(t)
            project(t, 0)

        @pl.when((t >= blocks) & (t < 2 * blocks))
        def _():
            project(t - blocks, 1)

        @pl.when(t == LAG - 1)
        def _():
            lax.fori_loop(0, table_ref.shape[0], fill_tables, 0)

        @pl.when((t >= LAG) & (t < blocks + LAG))
        def _():
            gather(t - LAG, 0)

        @pl.when(t >= blocks + LAG)
        def _():
            gather(t - blocks - LAG, 1)
        return carry

    lax.fori_loop(0, 2 * blocks + LAG, step, 0)
    far = SIDE * (PLANE - 1)
    for turn in range(2):
        for axis in range(3):
            span = spans[turn][axis]
            cols = slice(STARTS[axis] + span.start, STARTS[axis] + span.start + span.size)
            total = x_ref[:, cols].astype(F32) + sums[axis][0, :, span]
            for r in (2, 1, 3):
                wait_for(parts[axis].at[r - 1, :, span], line_recv.at[axis, turn * 3 + r - 1])
                total += parts[axis][r - 1, :, span]
            out_ref[:, cols] = total.astype(out_ref.dtype)
    for turn in range(2):
        for axis in range(3):
            span = spans[turn][axis]
            for r in range(1, SIDE):
                wait_for(sums[axis].at[r, :, span], line_send.at[axis, turn * 3 + r - 1])
            wait_for(rows[axis].at[pl.ds(0, far), :, span], send_sem.at[axis, turn])


def params(**kw):
    return pltpu.CompilerParams(vmem_limit_bytes=62 * 2 ** 20, **kw)


VMEM = pl.BlockSpec(memory_space=pltpu.VMEM)
ANY = pl.BlockSpec(memory_space=pl.ANY)
DMA = pltpu.SemaphoreType.DMA
shape = jax.ShapeDtypeStruct


def route(x_in, norm_gain, w_router, expert_ids):
    tokens, hidden = x_in.shape
    top_k = expert_ids.shape[1]
    return pl.pallas_call(
        route_kernel,
        out_shape=(shape((tokens, hidden), BF16), shape((top_k, tokens), F32)),
        compiler_params=params(),
        name="route",
    )(x_in, norm_gain.reshape(1, hidden), w_router, expert_ids, expert_ids.T)


def dispatch(h, ids_t, gates, devices):
    top_k, tokens = ids_t.shape
    table = shape((10, devices, tokens), F32)
    return pl.pallas_call(
        dispatch_kernel,
        out_shape=(table, table) + tuple(shape((devices, SLOTS, w), BF16) for w in WIDTHS),
        in_specs=[VMEM] * 3,
        out_specs=(VMEM, VMEM, ANY, ANY, ANY),
        scratch_shapes=[pltpu.VMEM((SIDE * SIDE, tokens, w), BF16) for w in WIDTHS]
        + [pltpu.VMEM((3, SIDE * SIDE, top_k, tokens), I32), pltpu.VMEM((9, top_k, tokens), F32)]
        + [pltpu.VMEM((devices, SLOTS, w), BF16) for w in WIDTHS]
        + [DMA((3,)), DMA((3, SIDE * SIDE)), DMA((3,)), DMA((3,)), DMA, DMA, DMA((3,)), DMA((3,)), DMA((3, SIDE * SIDE))],
        compiler_params=params(has_side_effects=True),
        name="dispatch",
    )(h, ids_t, gates)


def experts_mlp(x_in, post, gates, rows, w_gate, w_up, w_down):
    tokens, hidden = x_in.shape
    devices = rows[0].shape[0]
    out, *_ = pl.pallas_call(
        expert_kernel,
        out_shape=(shape((tokens, hidden), BF16),) + tuple(shape(r.shape, BF16) for r in rows),
        in_specs=[VMEM] * 3 + [ANY] * 3 + [VMEM] * 3,
        out_specs=(VMEM,) + (ANY,) * 3,
        scratch_shapes=[pltpu.VMEM((devices, SLOTS, w), BF16) for w in WIDTHS]
        + [pltpu.VMEM((16, SLOTS, w), BF16) for w in WIDTHS]
        + [pltpu.VMEM((SIDE, tokens, w), F32) for w in WIDTHS]
        + [pltpu.VMEM((3, tokens, w), F32) for w in WIDTHS]
        + [pltpu.VMEM((8, 16 * SLOTS, w_gate.shape[2]), BF16), pltpu.VMEM((10, 4 * tokens, devices), BF16)]
        + [DMA((3, 8)), DMA((3,)), DMA((3, 2)), DMA((3, 16)), DMA((3, 2 * SIDE)), DMA((3, 6)), DMA((3, 6))],
        compiler_params=params(has_side_effects=True),
        name="experts",
    )(x_in, post, gates, *rows, w_gate, w_up, w_down)
    return out


def solution(mesh):
    def local_block(x_in, norm_gain, w_router, expert_ids, w_gate, w_up, w_down):
        h, gates = route(x_in, norm_gain, w_router, expert_ids)
        post, dense, *rows = dispatch(h, expert_ids.T, gates, w_router.shape[1])
        return experts_mlp(x_in, post, dense, rows, w_gate, w_up, w_down)

    tok_spec = P(("dp", "ep"), None)
    expert_spec = P("ep", None, None)
    return jax.shard_map(local_block, mesh=mesh, in_specs=(tok_spec, P(None), P(None, None), tok_spec, expert_spec, expert_spec, expert_spec), out_specs=tok_spec, check_vma=False)
```

```python
import functools

import jax
import jax.numpy as jnp
from jax import lax
from jax.experimental import pallas as pl
from jax.experimental.pallas import tpu as pltpu
from jax.sharding import PartitionSpec as P

EPS = 1e-6
SLOTS = 32
SIDE = 4
STRIDES = (2, 8, 32)
WIDTHS = (768, 640, 640)
STARTS = (0, 768, 1408)
CUT = 384
PLANE = 32
LAG = 7
F32, BF16, I32 = jnp.float32, jnp.bfloat16, jnp.int32
MESH = pl.DeviceIdType.MESH


def shifted(dev, axis, step):
    stride = STRIDES[axis]
    here = lax.rem(lax.div(dev, stride), SIDE)
    return dev + (lax.rem(here + step, SIDE) - here) * stride


def plane_axes(axis):
    return tuple(a for a in (2, 1, 0) if a != axis)


def in_plane(dev, axis, p):
    a, b = plane_axes(axis)
    dev = shifted(shifted(dev, a, lax.div(p, 8)), b, lax.rem(lax.div(p, 2), SIDE))
    core = lax.rem(dev, 2)
    return dev + lax.rem(core + lax.rem(p, 2), 2) - core


def opposite(p):
    da, db = lax.div(p, 8), lax.rem(lax.div(p, 2), SIDE)
    return lax.rem(SIDE - da, SIDE) * 8 + lax.rem(SIDE - db, SIDE) * 2 + lax.rem(p, 2)


def bit(block, axis):
    return lax.rem(lax.div(block, 1 << axis), 2)


def member(axis, block, m):
    a, b = plane_axes(axis)
    return (bit(block, a) + 2 * lax.div(m, 4)) * 8 + (bit(block, b) + 2 * lax.rem(lax.div(m, 2), 2)) * 2 + lax.rem(m, 2)


def place_of(step, core):
    odd = (lax.rem(step[2], 2) * 2 + lax.rem(step[1], 2)) * 2 + lax.rem(step[0], 2)
    half = (lax.div(step[2], 2) * 2 + lax.div(step[1], 2)) * 2 + lax.div(step[0], 2)
    return odd * 16 + half * 2 + core


def split_place(axis, place):
    block, half = lax.div(place, 16), lax.div(lax.rem(place, 16), 2)
    step = tuple(bit(block, i) + 2 * bit(half, i) for i in range(3))
    a, b = plane_axes(axis)
    return step[axis], step[a] * 8 + step[b] * 2 + lax.rem(place, 2)


def remote(src, dst, send_sem, recv_sem, dev):
    return pltpu.make_async_remote_copy(src, dst, send_sem, recv_sem, device_id={"ep": dev}, device_id_type=MESH)


def wait_for(ref, sem):
    pltpu.make_async_copy(ref, ref, sem).wait()


def source(axis, r):
    return 0 if r == 0 else 3 * axis + r


def place_in_tables(axis, r):
    return (3 * axis + r) * lax.min(r, 1)


def route_kernel(x_ref, gain_ref, wr_ref, ids_ref, idst_ref, h_ref, gate_ref):
    tokens, experts = x_ref.shape[0], wr_ref.shape[1]
    top_k = ids_ref.shape[1]
    resid = x_ref[...].astype(F32)
    mean_sq = jnp.mean(resid * resid, axis=-1, keepdims=True)
    normed = (resid * lax.rsqrt(mean_sq + EPS) * gain_ref[...].astype(F32)).astype(BF16)
    h_ref[...] = normed
    logits = jnp.dot(normed, wr_ref[...], preferred_element_type=F32)
    exps = jnp.exp(logits - jnp.max(logits, axis=-1, keepdims=True))
    router_p = exps / jnp.sum(exps, axis=-1, keepdims=True)
    lane_expert = lax.broadcasted_iota(I32, (tokens, experts), 1)
    chosen = jnp.zeros((tokens, experts), F32)
    for j in range(top_k):
        chosen += jnp.where(ids_ref[:, j:j + 1] == lane_expert, 1.0, 0.0)
    picked = router_p * chosen
    gates_t = jnp.transpose(picked / jnp.sum(picked, axis=-1, keepdims=True))
    row_expert = lax.broadcasted_iota(I32, (experts, tokens), 0)
    for j in range(top_k):
        gate_ref[j:j + 1, :] = jnp.sum(jnp.where(idst_ref[j:j + 1, :] == row_expert, gates_t, 0.0), axis=0, keepdims=True)


def dispatch_kernel(h_ref, ids_ref, gate_ref, post_ref, gates_ref, recv0, recv1, recv2,
                    line0, line1, line2, ids_scr, gate_scr, pack0, pack1, pack2,
                    line_send, line_recv, ids_send, ids_recv, gate_send, gate_recv, send_sem, recv_sem, local_sem):
    recv, line, pack = (recv0, recv1, recv2), (line0, line1, line2), (pack0, pack1, pack2)
    top_k, tokens = ids_ref.shape
    experts = post_ref.shape[1]
    me = lax.axis_index("ep")

    def forward(axis, r, src):
        for q in (1, 3):
            n = r * SIDE + SIDE - q
            remote(src, line[axis].at[n], line_send.at[axis], line_recv.at[axis, n], shifted(me, (axis + 1) % 3, q)).start()

    def pass_on(axis, r, q, first):
        part, n = pl.ds(first, tokens // 2), r * SIDE + 2
        remote(line[axis].at[r * SIDE + q, part], line[axis].at[n, part], line_send.at[axis], line_recv.at[axis, n], shifted(me, (axis + 1) % 3, SIDE - q)).start()

    def pass_along(axis, r, first):
        part, n = pl.ds(first, tokens // 2), 2 * SIDE
        remote(line[axis].at[r * SIDE, part], line[axis].at[n, part], line_send.at[axis], line_recv.at[axis, n], shifted(me, axis, SIDE - r)).start()

    for axis in range(3):
        for n in range(1, SIDE * SIDE):
            r, q = n // SIDE, n % SIDE
            dev = shifted(shifted(me, axis, r), (axis + 1) % 3, q)
            there = ((SIDE - r) % SIDE) * SIDE + (SIDE - q) % SIDE
            remote(ids_ref, ids_scr.at[axis, there], ids_send.at[axis], ids_recv.at[axis], dev).start()
    for r in (1, 3):
        for axis in range(3):
            n = (SIDE - r) * SIDE
            src = h_ref.at[:, pl.ds(STARTS[axis], WIDTHS[axis])]
            remote(src, line[axis].at[n], line_send.at[axis], line_recv.at[axis, n], shifted(me, axis, r)).start()
    for axis in range(3):
        forward(axis, 0, h_ref.at[:, pl.ds(STARTS[axis], WIDTHS[axis])])
    for axis in range(3):
        for r in range(1, SIDE):
            k = 3 * axis + SIDE - r - 1
            remote(gate_ref, gate_scr.at[k], gate_send, gate_recv, shifted(me, axis, r)).start()
        line[axis][0] = h_ref[:, STARTS[axis]:STARTS[axis] + WIDTHS[axis]]
        ids_scr[axis, 0] = ids_ref[...]

    row_expert = lax.broadcasted_iota(I32, (experts, tokens), 0)
    rows = lax.broadcasted_iota(I32, (tokens, tokens), 0)
    upper = jnp.where(rows < lax.broadcasted_iota(I32, (tokens, tokens), 1), 1.0, 0.0).astype(BF16)
    slot = lax.broadcasted_iota(I32, (8, SLOTS, tokens), 1).astype(F32)
    eight = lax.broadcasted_iota(I32, (8, tokens), 0)

    def across(axis, m):
        dev = shifted(me, (axis + 2) % 3, lax.div(m, 2))
        core = lax.rem(dev, 2)
        return dev + lax.rem(core + lax.rem(m, 2), 2) - core

    def swap(v):
        return v + lax.div(v, 2) * (5 - 2 * v)

    def step(t, carry):
        r, q = swap(lax.rem(t, SIDE)), swap(lax.div(t, SIDE))
        n = r * SIDE + q
        for axis in range(3):
            @pl.when(t == 1)
            def _():
                wait_for(ids_scr.at[axis, pl.ds(1, SIDE * SIDE - 1)], ids_recv.at[axis])

            @pl.when(t > 0)
            def _():
                wait_for(line[axis].at[n], line_recv.at[axis, n])

            @pl.when((t > 0) & (t < SIDE))
            def _():
                forward(axis, r, line[axis].at[n])

            @pl.when(t == 1)
            def _():
                pass_along(axis, 1, tokens // 2)

            @pl.when(t == 2)
            def _():
                pass_along(axis, 3, 0)

            @pl.when((t >= SIDE) & (t < 2 * SIDE))
            def _():
                pass_on(axis, r, 1, tokens // 2)

            @pl.when((t >= 2 * SIDE) & (t < 3 * SIDE))
            def _():
                pass_on(axis, r, 3, 0)

            theirs = across(axis, eight)
            chosen = jnp.zeros((8, tokens), F32)
            for j in range(top_k):
                chosen += jnp.where(ids_scr[axis, n, j:j + 1, :] == theirs, 1.0, 0.0)
            before = jnp.dot(chosen.astype(BF16), upper, preferred_element_type=F32)
            post = jnp.where(chosen > 0.0, before, 255.0)
            pick = jnp.where(post[:, None, :] == slot, 1.0, 0.0).astype(BF16).reshape(8 * SLOTS, tokens)
            packed = jnp.dot(pick, line[axis][n], preferred_element_type=F32).astype(BF16)
            pack[axis][pl.ds(t * 8, 8)] = packed.reshape(8, SLOTS, WIDTHS[axis])

        def send(i, c):
            m = lax.rem(i + 2, 8)
            for axis in range(3):
                steps = {axis: r, (axis + 1) % 3: q, (axis + 2) % 3: lax.rem(SIDE - lax.div(m, 2), SIDE)}
                src = pack[axis].at[t * 8 + m]
                dst = recv[axis].at[place_of(steps, lax.rem(m, 2))]

                @pl.when(m == 0)
                def _():
                    pltpu.make_async_copy(src, dst, local_sem.at[axis, t]).start()

                @pl.when(m != 0)
                def _():
                    remote(src, dst, send_sem.at[axis], recv_sem.at[axis], across(axis, m)).start()
            return c

        lax.fori_loop(0, 8, send, 0)
        return carry

    steps = SIDE * SIDE
    lax.fori_loop(0, steps, step, 0)

    def tables(k, ids, gates):
        chosen = jnp.zeros((experts, tokens), F32)
        dense = jnp.zeros((experts, tokens), F32)
        for j in range(top_k):
            hit = ids[j:j + 1, :] == row_expert
            chosen += jnp.where(hit, 1.0, 0.0)
            dense += jnp.where(hit, gates[j:j + 1, :], 0.0)
        before = jnp.dot(chosen.astype(BF16), upper, preferred_element_type=F32)
        post_ref[k] = jnp.where(chosen > 0.0, before, 255.0)
        gates_ref[k] = dense

    wait_for(gate_scr, gate_recv)
    tables(0, ids_ref[...], gate_ref[...])
    for axis in range(3):
        for r in range(1, SIDE):
            k = source(axis, r)
            tables(k, ids_scr[axis, r * SIDE], gate_scr[k - 1])

    wait_for(gate_scr, gate_send)
    for axis in range(3):
        wait_for(ids_scr.at[axis, pl.ds(1, steps - 1)], ids_send.at[axis])
        wait_for(line[axis].at[pl.ds(1, steps - 1)], line_send.at[axis])
        for t in range(steps):
            wait_for(recv[axis].at[0], local_sem.at[axis, t])
        wait_for(pack[axis].at[pl.ds(0, 7 * steps)], send_sem.at[axis])
        wait_for(recv[axis].at[pl.ds(0, 7 * steps)], recv_sem.at[axis])


def expert_kernel(x_ref, post_ref, gates_ref, x0, x1, x2, wg_ref, wu_ref, wd_ref, out_ref, ret0, ret1, ret2,
                  row0, row1, row2, in0, in1, in2, sum0, sum1, sum2, part0, part1, part2, act_ref, table_ref,
                  load_sem, back_sem, send_sem, recv_sem, local_sem, line_send, line_recv):
    x, ret, rows, held = (x0, x1, x2), (ret0, ret1, ret2), (row0, row1, row2), (in0, in1, in2)
    sums, parts = (sum0, sum1, sum2), (part0, part1, part2)
    me = lax.axis_index("ep")
    tokens, experts = x_ref.shape[0], post_ref.shape[1]
    blocks, size, width = 8, 16, 8 * SLOTS
    spans = [[pl.ds(0, CUT) for w in WIDTHS], [pl.ds(CUT, w - CUT) for w in WIDTHS]]

    def load(b, axis):
        part = pl.ds(b * size, size)
        return pltpu.make_async_copy(x[axis].at[part], rows[axis].at[part], load_sem.at[axis, b])

    for b in range(blocks):
        for axis in range(3):
            load(b, axis).start()
    for axis in range(3):
        sums[axis][...] = jnp.zeros(sums[axis].shape, F32)

    def activate(b):
        for axis in range(3):
            load(b, axis).wait()
        gate_val, up_val = 0.0, 0.0
        for axis in range(3):
            part = rows[axis][pl.ds(b * size, size)].reshape(size * SLOTS, WIDTHS[axis])
            span = slice(STARTS[axis], STARTS[axis] + WIDTHS[axis])
            gate_val += jnp.dot(part, wg_ref[0, span, :], preferred_element_type=F32)
            up_val += jnp.dot(part, wu_ref[0, span, :], preferred_element_type=F32)
        act_ref[b] = (jax.nn.silu(gate_val) * up_val).astype(BF16)

    def project(b, turn):
        for axis in range(3):
            span = spans[turn][axis]
            y = jnp.dot(act_ref[b], wd_ref[0, :, pl.ds(STARTS[axis] + span.start, span.size)], preferred_element_type=F32).astype(BF16)
            rows[axis][pl.ds(b * size, size), :, span] = y.reshape(size, SLOTS, span.size)

        def send(j, c):
            place = b * size + j
            for axis in range(3):
                along, p = split_place(axis, place)
                src, dst = rows[axis].at[place, :, spans[turn][axis]], ret[axis].at[place, :, spans[turn][axis]]

                @pl.when(p == 0)
                def _():
                    pltpu.make_async_copy(src, dst, local_sem.at[axis, turn * SIDE + along]).start()

                @pl.when(p != 0)
                def _():
                    remote(src, dst, send_sem.at[axis, turn], recv_sem.at[axis, turn * blocks + b], in_plane(me, axis, p)).start()
            return c

        lax.fori_loop(0, size, send, 0)

    def fill_tables(k, c):
        gates = jnp.transpose(gates_ref[k])
        high = gates.astype(BF16)
        rest = gates - high.astype(F32)
        mid = rest.astype(BF16)
        low = (rest - mid.astype(F32)).astype(BF16)
        table_ref[k] = jnp.concatenate([high, mid, low, jnp.transpose(post_ref[k]).astype(BF16)], axis=0)
        return c

    def partial(axis, r, turn):
        span = spans[turn][axis]
        return remote(sums[axis].at[r, :, span], parts[axis].at[SIDE - r - 1, :, span], line_send.at[axis, turn * 3 + r - 1], line_recv.at[axis, turn * 3 + SIDE - r - 1], shifted(me, axis, r))

    expert = lax.broadcasted_iota(I32, (experts, width), 0)
    column = lax.div(lax.broadcasted_iota(I32, (1, width), 1), SLOTS)
    slot = lax.rem(lax.broadcasted_iota(I32, (1, width), 1), SLOTS).astype(F32)

    def gather(b, turn):
        def back(axis):
            span = spans[turn][axis]
            return pltpu.make_async_copy(ret[axis].at[pl.ds(b * size, size), :, span], held[axis].at[:, :, span], back_sem.at[axis])

        for axis in range(3):
            a1, a2 = plane_axes(axis)
            odd, span = bit(b, axis), spans[turn][axis]
            near = bit(b, a1) + bit(b, a2) == 0

            @pl.when(near)
            def _():
                wait_for(ret[axis].at[0, :, span], local_sem.at[axis, turn * SIDE + odd])
                wait_for(ret[axis].at[0, :, span], local_sem.at[axis, turn * SIDE + odd + 2])
                wait_for(ret[axis].at[pl.ds(0, size - 2), :, span], recv_sem.at[axis, turn * blocks + b])

            @pl.when(jnp.logical_not(near))
            def _():
                wait_for(ret[axis].at[pl.ds(0, size), :, span], recv_sem.at[axis, turn * blocks + b])

            back(axis).start()
        for axis in range(3):
            span = spans[turn][axis]
            back(axis).wait()
            theirs = in_plane(me, axis, opposite(member(axis, b, column)))
            spread = jnp.where(theirs == expert, 1.0, 0.0).astype(BF16)
            for two in range(2):
                r = bit(b, axis) + 2 * two
                wide = jnp.dot(table_ref[place_in_tables(axis, r)], spread, preferred_element_type=F32)
                hit = wide[3 * tokens:] == slot
                weight = jnp.concatenate([jnp.where(hit, wide[i * tokens:(i + 1) * tokens], 0.0).astype(BF16) for i in range(3)], axis=0)
                run = 2 << axis
                pieces = [held[axis][i:i + run, :, span].reshape(run * SLOTS, span.size) for i in range(two * run, size, 2 * run)]
                got = jnp.dot(weight, jnp.concatenate(pieces, axis=0), preferred_element_type=F32)
                sums[axis][r, :, span] += got[:tokens] + got[tokens:2 * tokens] + got[2 * tokens:]
        for axis in range(3):
            @pl.when(b == 7 - (1 << axis))
            def _():
                partial(axis, 2, turn).start()

            @pl.when(b == 7)
            def _():
                partial(axis, 1, turn).start()
                partial(axis, 3, turn).start()

    def step(t, carry):
        @pl.when(t < blocks)
        def _():
            activate(t)
            project(t, 0)

        @pl.when((t >= blocks) & (t < 2 * blocks))
        def _():
            project(t - blocks, 1)

        @pl.when(t == LAG - 1)
        def _():
            lax.fori_loop(0, table_ref.shape[0], fill_tables, 0)

        @pl.when((t >= LAG) & (t < blocks + LAG))
        def _():
            gather(t - LAG, 0)

        @pl.when(t >= blocks + LAG)
        def _():
            gather(t - blocks - LAG, 1)
        return carry

    lax.fori_loop(0, 2 * blocks + LAG, step, 0)
    far = SIDE * (PLANE - 1)
    for turn in range(2):
        for axis in range(3):
            span = spans[turn][axis]
            cols = slice(STARTS[axis] + span.start, STARTS[axis] + span.start + span.size)
            total = x_ref[:, cols].astype(F32) + sums[axis][0, :, span]
            for r in (2, 1, 3):
                wait_for(parts[axis].at[r - 1, :, span], line_recv.at[axis, turn * 3 + r - 1])
                total += parts[axis][r - 1, :, span]
            out_ref[:, cols] = total.astype(out_ref.dtype)
    for turn in range(2):
        for axis in range(3):
            span = spans[turn][axis]
            for r in range(1, SIDE):
                wait_for(sums[axis].at[r, :, span], line_send.at[axis, turn * 3 + r - 1])
            wait_for(rows[axis].at[pl.ds(0, far), :, span], send_sem.at[axis, turn])


def params(**kw):
    return pltpu.CompilerParams(vmem_limit_bytes=62 * 2 ** 20, **kw)


VMEM = pl.BlockSpec(memory_space=pltpu.VMEM)
ANY = pl.BlockSpec(memory_space=pl.ANY)
DMA = pltpu.SemaphoreType.DMA
shape = jax.ShapeDtypeStruct


def route(x_in, norm_gain, w_router, expert_ids):
    tokens, hidden = x_in.shape
    top_k = expert_ids.shape[1]
    return pl.pallas_call(
        route_kernel,
        out_shape=(shape((tokens, hidden), BF16), shape((top_k, tokens), F32)),
        compiler_params=params(),
        name="route",
    )(x_in, norm_gain.reshape(1, hidden), w_router, expert_ids, expert_ids.T)


def dispatch(h, ids_t, gates, devices):
    top_k, tokens = ids_t.shape
    table = shape((10, devices, tokens), F32)
    return pl.pallas_call(
        dispatch_kernel,
        out_shape=(table, table) + tuple(shape((devices, SLOTS, w), BF16) for w in WIDTHS),
        in_specs=[VMEM] * 3,
        out_specs=(VMEM, VMEM, ANY, ANY, ANY),
        scratch_shapes=[pltpu.VMEM((SIDE * SIDE, tokens, w), BF16) for w in WIDTHS]
        + [pltpu.VMEM((3, SIDE * SIDE, top_k, tokens), I32), pltpu.VMEM((9, top_k, tokens), F32)]
        + [pltpu.VMEM((devices, SLOTS, w), BF16) for w in WIDTHS]
        + [DMA((3,)), DMA((3, SIDE * SIDE)), DMA((3,)), DMA((3,)), DMA, DMA, DMA((3,)), DMA((3,)), DMA((3, SIDE * SIDE))],
        compiler_params=params(has_side_effects=True),
        name="dispatch",
    )(h, ids_t, gates)


def experts_mlp(x_in, post, gates, rows, w_gate, w_up, w_down):
    tokens, hidden = x_in.shape
    devices = rows[0].shape[0]
    out, *_ = pl.pallas_call(
        expert_kernel,
        out_shape=(shape((tokens, hidden), BF16),) + tuple(shape(r.shape, BF16) for r in rows),
        in_specs=[VMEM] * 3 + [ANY] * 3 + [VMEM] * 3,
        out_specs=(VMEM,) + (ANY,) * 3,
        scratch_shapes=[pltpu.VMEM((devices, SLOTS, w), BF16) for w in WIDTHS]
        + [pltpu.VMEM((16, SLOTS, w), BF16) for w in WIDTHS]
        + [pltpu.VMEM((SIDE, tokens, w), F32) for w in WIDTHS]
        + [pltpu.VMEM((3, tokens, w), F32) for w in WIDTHS]
        + [pltpu.VMEM((8, 16 * SLOTS, w_gate.shape[2]), BF16), pltpu.VMEM((10, 4 * tokens, devices), BF16)]
        + [DMA((3, 8)), DMA((3,)), DMA((3, 2)), DMA((3, 16)), DMA((3, 2 * SIDE)), DMA((3, 6)), DMA((3, 6))],
        compiler_params=params(has_side_effects=True),
        name="experts",
    )(x_in, post, gates, *rows, w_gate, w_up, w_down)
    return out


def solution(mesh):
    def local_block(x_in, norm_gain, w_router, expert_ids, w_gate, w_up, w_down):
        h, gates = route(x_in, norm_gain, w_router, expert_ids)
        post, dense, *rows = dispatch(h, expert_ids.T, gates, w_router.shape[1])
        return experts_mlp(x_in, post, dense, rows, w_gate, w_up, w_down)

    tok_spec = P(("dp", "ep"), None)
    expert_spec = P("ep", None, None)
    return jax.shard_map(local_block, mesh=mesh, in_specs=(tok_spec, P(None), P(None, None), tok_spec, expert_spec, expert_spec, expert_spec), out_specs=tok_spec, check_vma=False)
```
